32 devices in a mesh: rep: 8 (over y, x, core), tp: 4 (over z).
Axes of the slice: x: 2, y: 2, z: 4, core: 2. Of those that a mesh axis runs over, the one named last changes fastest.
Arguments:
- hidden: bfloat16 [512, 8192], P('rep'), may hold values from -6 to 6
- norm_gain: bfloat16 [8192], replicated, may hold values from 0.5 to 1.5
- query_weight_matrix: bfloat16 [8192, 4096], P(None, 'tp'), may hold values from -0.0625 to 0.0625
- key_value_weight: bfloat16 [2, 8192, 1024], P(None, None, 'tp'), may hold values from -0.0625 to 0.0625
- output_weight_matrix: bfloat16 [4096, 8192], P('tp'), may hold values from -0.375 to 0.375
- input_down_factors: bfloat16 [3, 8192, 64], P(None, ('rep', 'tp')), may hold values from -0.0625 to 0.0625
- query_up_factor: bfloat16 [64, 4096], P(None, ('rep', 'tp')), may hold values from -0.75 to 0.75
- key_value_up_factors: bfloat16 [2, 64, 1024], P(None, None, ('rep', 'tp')), may hold values from -0.75 to 0.75
- output_down_factor: bfloat16 [4096, 64], P(('rep', 'tp')), may hold values from -0.375 to 0.375
- output_up_factor: bfloat16 [64, 8192], P(None, ('rep', 'tp')), may hold values from -0.75 to 0.75
- cache_keys: bfloat16 [512, 8, 128, 128], P('rep', 'tp'), may hold values from -360 to 360
- cache_values: bfloat16 [512, 8, 128, 128], P('rep', 'tp'), may hold values from -6 to 6
- lengths: int32 [512], P('rep'), may hold values from 1 to 127
Outputs:
- attn_out: bfloat16 [512, 8192], P('rep', 'tp')
The draws below stay inside these ranges and needn't reach their ends.
All inputs are finite; a program needn't handle non-finite values.
Results may differ from the reference program's by a relative error of at most 0.03.
Values may be sent and summed in bfloat16 or wider, within the bound.
A program may use at most 128 MiB of HBM per device.

```python
import math
import jax
import jax.numpy as jnp
from jax import lax

D = 8192
HEADS = 32
KV_HEADS = 8
HEAD_DIM = 128
RANK = 64
CACHE = 128
BATCH = 512


def draw_cache_keys(key, part):
    base_key = jax.random.fold_in(key, 11)
    values = jax.random.normal(base_key, (BATCH, KV_HEADS, CACHE, HEAD_DIM), jnp.float32)
    values = jnp.clip(values, -6.0, 6.0)
    return values.astype(jnp.bfloat16)


def set_ends(array, key, least, largest):
    spot = [jax.random.randint(jax.random.fold_in(key, axis), (), 0, length) for axis, length in enumerate(array.shape)]
    widest = array.shape.index(max(array.shape))
    next_to = spot[:widest] + [(spot[widest] + 1) % array.shape[widest]] + spot[widest + 1:]
    return array.at[tuple(spot)].set(least).at[tuple(next_to)].set(largest)


def levels(stream_key, dims, shards, least, largest):
    factor_of, own = 1.0, jax.random.fold_in(stream_key, 6)
    for axis_at, blocks in shards:
        heights = jnp.exp(jax.random.uniform(jax.random.fold_in(own, axis_at), (blocks,), jnp.float32, least / len(shards), largest / len(shards)))
        factor_of = factor_of * jnp.repeat(heights, dims[axis_at] // blocks).reshape([-1 if axis == axis_at else 1 for axis in range(len(dims))])
    return factor_of


def normal_values(rng, extent, scale, most, pieces=(), held_as=jnp.bfloat16):
    entries = jax.random.normal(rng, extent, jnp.float32) * scale
    if len(pieces) > 0:
        entries = levels(rng, extent, pieces, -0.22, 0.18) * entries
    return jnp.clip(entries, min=-most, max=most).astype(held_as)


def setup_inputs(seed: int = 0) -> dict:
    key_list = jax.random.split(jax.random.key(seed), 14)
    hidden = normal_values(key_list[0], (BATCH, D), 1.0, 6.0, ((0, 8),))
    norm_gain = jnp.clip(1.0 + 0.1 * jax.random.normal(key_list[1], (D,), jnp.float32), 0.5, 1.5).astype(jnp.bfloat16)
    query_weight_matrix = normal_values(key_list[2], (D, HEADS * HEAD_DIM), D ** -0.5, 0.0625, ((1, 4),))
    key_value_weight = normal_values(key_list[3], (2, D, KV_HEADS * HEAD_DIM), D ** -0.5, 0.0625, ((2, 4),))
    output_weight_matrix = normal_values(key_list[4], (HEADS * HEAD_DIM, D), (HEADS * HEAD_DIM // 16) ** -0.5, 0.375, ((0, 4),))
    input_down_factors = normal_values(key_list[5], (3, D, RANK), D ** -0.5, 0.0625, ((1, 32),))
    query_up_factor = normal_values(key_list[6], (RANK, HEADS * HEAD_DIM), RANK ** -0.5, 0.75, ((1, 32),))
    key_value_up_factors = normal_values(key_list[7], (2, RANK, KV_HEADS * HEAD_DIM), RANK ** -0.5, 0.75, ((2, 32),))
    output_down_factor = normal_values(key_list[8], (HEADS * HEAD_DIM, RANK), (HEADS * HEAD_DIM // 16) ** -0.5, 0.375, ((0, 32),))
    output_up_factor = normal_values(key_list[9], (RANK, D), RANK ** -0.5, 0.75, ((1, 32),))
    cache_keys = draw_cache_keys(jax.random.fold_in(key_list[13], 71), 0)
    cache_values = normal_values(key_list[11], (BATCH, KV_HEADS, CACHE, HEAD_DIM), 1.0, 6.0, ((0, 8), (1, 4)))
    lengths = set_ends(jax.random.randint(key_list[12], (BATCH,), 1, CACHE), jax.random.fold_in(key_list[12], 1), 1, CACHE - 1).astype(jnp.int32)
    return dict(hidden=hidden, norm_gain=norm_gain, query_weight_matrix=query_weight_matrix, key_value_weight=key_value_weight, output_weight_matrix=output_weight_matrix, input_down_factors=input_down_factors, query_up_factor=query_up_factor, key_value_up_factors=key_value_up_factors, output_down_factor=output_down_factor, output_up_factor=output_up_factor, cache_keys=cache_keys, cache_values=cache_values, lengths=lengths)


epsilon = 1e-06
rope_base = 1000000.0
adapter_scale = 0.5

def rope_angles(lengths, head_dim):
    half_dim = head_dim // 2
    frequency = rope_base ** (-(jnp.arange(half_dim, dtype=jnp.float32) * 2.0) / head_dim)
    return lengths.astype(jnp.float32)[:, None] * frequency[None, :]

def rotate(vectors, angles):
    half_dim = vectors.shape[-1] // 2
    cosine = jnp.cos(angles)[:, None, :]
    sine_part = jnp.sin(angles)[:, None, :]
    low_half = vectors[..., :half_dim]
    high_half = vectors[..., half_dim:]
    return jnp.concatenate([low_half * cosine - high_half * sine_part, high_half * cosine + low_half * sine_part], axis=-1)

def adapted(normed, frozen_matrix, inner_part, up_factor):
    base_part = jnp.dot(normed, frozen_matrix, preferred_element_type=jnp.float32)
    return base_part + adapter_scale * jnp.dot(inner_part, up_factor, preferred_element_type=jnp.float32)

def attend(query, new_key, new_value, keys, values, lengths):
    score_scale = 1.0 / math.sqrt(keys.shape[-1])
    scores = jnp.einsum('bkgd,bkld->bkgl', query, keys.astype(jnp.float32), precision=lax.Precision.HIGHEST) * score_scale
    own_score = lax.optimization_barrier(jnp.sum(query * new_key.astype(jnp.float32)[:, :, None, :], axis=-1)) * score_scale
    live_mask = jnp.arange(keys.shape[2], dtype=jnp.int32)[None, None, None, :] < lengths[:, None, None, None]
    row_max = jnp.maximum(lax.optimization_barrier(jnp.max(jnp.where(live_mask, scores, -1e+30), axis=-1)), own_score)
    weights = jnp.where(live_mask, jnp.exp(scores - row_max[..., None]), 0.0)
    own_weight = jnp.exp(own_score - row_max)
    denom_sum = lax.optimization_barrier(jnp.sum(weights, axis=-1)) + own_weight
    probs = (weights / denom_sum[..., None]).astype(jnp.bfloat16)
    own_prob = (own_weight / denom_sum).astype(jnp.bfloat16)
    context = jnp.einsum('bkgl,bkld->bkgd', probs.astype(jnp.float32), values.astype(jnp.float32))
    context = context + own_prob.astype(jnp.float32)[..., None] * new_value.astype(jnp.float32)[:, :, None, :]
    return context.astype(jnp.bfloat16)

def reference(hidden, norm_gain, query_weight_matrix, key_value_weight, output_weight_matrix, input_down_factors, query_up_factor, key_value_up_factors, output_down_factor, output_up_factor, cache_keys, cache_values, lengths):
    states = hidden.astype(jnp.float32)
    square = lax.optimization_barrier(jnp.mean(states * states, axis=-1, keepdims=True))
    normed = (states * lax.rsqrt(square + epsilon) * norm_gain.astype(jnp.float32)).astype(jnp.bfloat16)
    inner_query = jnp.dot(normed, input_down_factors[0], preferred_element_type=jnp.float32).astype(jnp.bfloat16)
    inner_key = jnp.dot(normed, input_down_factors[1], preferred_element_type=jnp.float32).astype(jnp.bfloat16)
    inner_value = jnp.dot(normed, input_down_factors[2], preferred_element_type=jnp.float32).astype(jnp.bfloat16)
    batch = hidden.shape[0]
    kv_count = cache_keys.shape[1]
    head_dim = cache_keys.shape[3]
    angles = rope_angles(lengths, head_dim)
    query = adapted(normed, query_weight_matrix, inner_query, query_up_factor).reshape(batch, -1, head_dim)
    query = rotate(query, angles).reshape(batch, kv_count, -1, head_dim)
    new_key = adapted(normed, key_value_weight[0], inner_key, key_value_up_factors[0]).reshape(batch, kv_count, head_dim)
    new_key = rotate(new_key, angles).astype(jnp.bfloat16)
    new_value = adapted(normed, key_value_weight[1], inner_value, key_value_up_factors[1]).reshape(batch, kv_count, head_dim).astype(jnp.bfloat16)
    context = attend(query, new_key, new_value, cache_keys, cache_values, lengths).reshape(batch, -1)
    middle = jnp.dot(context, output_down_factor, preferred_element_type=jnp.float32).astype(jnp.bfloat16)
    return adapted(context, output_weight_matrix, middle, output_up_factor).astype(jnp.bfloat16)
```

```python
import functools
import math

import jax
import jax.numpy as jnp
from jax import lax
from jax.experimental import pallas as pl
from jax.experimental.pallas import tpu as pltpu
from jax.sharding import PartitionSpec as P

epsilon = 1e-06
rope_base = 1000000.0
adapter_scale = 0.5

f32 = jnp.float32
bf16 = jnp.bfloat16
LANES = 128
MESH_ID = pl.DeviceIdType.MESH


def nt_dot(left, right):
    return lax.dot_general(
        left, right, (((1,), (1,)), ((), ())), preferred_element_type=f32
    )


def nn_dot(left, right):
    return jnp.dot(left, right, preferred_element_type=f32)


def channels_of(n):
    return ((1, 0, n // 2), (-1, 1, n // 2), (1, 1, n // 2 - 1), (-1, 0, n // 2 - 1))


def kernel(
    dims,
    hidden,
    gain,
    wq,
    wkv,
    wo,
    dn_own,
    v_own,
    cache_k,
    cache_v,
    lengths,
    cos,
    sin,
    out,
    hid_b,
    norm_b,
    wq_b,
    wkv_b,
    wo_b,
    k_b,
    v_b,
    dn_b,
    vo_b,
    vf_b,
    q_acc,
    kv_acc,
    inner_s,
    inner_r,
    q3,
    nk3,
    nv3,
    c3,
    ctx,
    mid_s,
    mid_r,
    rs_s,
    rs_r,
    hid_sem,
    w_sem,
    kv_sem,
    wo_sem,
    k_sem,
    v_sem,
    own_sem,
    dn_ssem,
    dn_rsem,
    dn_fsem,
    vf_ssem,
    vf_rsem,
    vf_fsem,
    in_ssem,
    in_rsem,
    mid_ssem,
    mid_rsem,
    rs_ssem,
    rs_rsem,
):
    n, reps = dims["tp"], dims["rep"]
    seqs, depth = hidden.shape
    head_dim = cache_k.shape[3]
    kv_local = cache_k.shape[1]
    heads = wq.shape[1] // head_dim
    group = heads // kv_local
    pad_heads = q3.shape[0] // seqs
    rank = dims["rank"]
    block, win = dims["block"], dims["win"]
    q_rows, up_rows, kv_rows = dims["q_rows"], dims["up_rows"], dims["kv_rows"]
    half_reps = reps // 2
    r = lax.axis_index("rep")
    t = lax.axis_index("tp")
    core = lax.rem(r, 2)
    partner = r + 1 - 2 * core

    own_dn = pltpu.make_async_copy(dn_own, dn_b.at[r], own_sem.at[0])
    own_v = pltpu.make_async_copy(v_own, vo_b, own_sem.at[1])
    own_dn.start()
    own_v.start()
    hid = pltpu.make_async_copy(hidden, hid_b, hid_sem)
    hid.start()
    steps = w_sem.shape[0]
    kc = depth // steps

    def w_copies(i):
        rows = pl.ds(pl.multiple_of(i * kc, kc), kc)
        return (
            pltpu.make_async_copy(wq.at[rows, :], wq_b.at[rows, :], w_sem.at[i]),
            pltpu.make_async_copy(wkv.at[:, rows, :], wkv_b.at[:, rows, :], kv_sem.at[i]),
        )

    @pl.loop(0, steps)
    def _(i):
        for c in w_copies(i):
            c.start()

    parts = k_sem.shape[0]
    ps = seqs // parts

    def cache_copies(i):
        rows = pl.ds(i * ps, ps)
        return (
            pltpu.make_async_copy(cache_k.at[rows], k_b.at[rows], k_sem.at[i]),
            pltpu.make_async_copy(cache_v.at[rows], v_b.at[rows], v_sem.at[i]),
        )

    @pl.loop(0, parts)
    def _(i):
        for c in cache_copies(i):
            c.start()

    wide = wo.shape[1] // n
    half_w = wide // 2

    def out_cols(k, half):
        d = lax.rem(t + k + n, n)
        return pl.ds(pl.multiple_of(d * wide + half * half_w, LANES), half_w)

    def wo_copy(k, half):
        cols = out_cols(k, half)
        idx = (k % n) * 2 + half
        return pltpu.make_async_copy(wo.at[:, cols], wo_b.at[idx], wo_sem.at[idx])

    sends = []
    for k in range(n // 2, 0, -1):
        for fresh in (True, False):
            for ci, (way, half, hops) in enumerate(channels_of(n)):
                if k <= hops and (k == hops) == fresh:
                    sends.append((ci, way, half, hops, k))
    for _ci, way, half, _hops, k in sends:
        wo_copy(way * k, half).start()
    wo_copy(0, 0).start()
    wo_copy(0, 1).start()

    flat = r * n + t
    plane = flat // reps
    slot = lax.rem(flat, reps)
    barrier = pltpu.get_barrier_semaphore()

    def greet(rr, tt):
        pl.semaphore_signal(barrier, inc=1, device_id=(rr, tt), device_id_type=MESH_ID)

    count = 0
    greet(partner, t)
    count += 1
    for j in range(1, n):
        greet(r, lax.rem(t + j, n))
        count += 1
    for j in range(1, half_reps):
        greet(lax.rem(r + 2 * j, reps), t)
        count += 1
        greet(lax.rem(r + 2 * j, reps), plane)
        count += 1

    greet(jnp.where(plane == t, partner, r), plane)
    count += 1
    groups = reps // n // 2

    def source_of(i, z):
        s = n * (2 * i + core) + z
        return s, (reps * t + s) // n

    for i in range(groups):
        for z in range(n):
            _s, sr = source_of(i, z)
            same = jnp.logical_and(sr == r, t == z)
            greet(jnp.where(same, partner, sr), z)
            count += 1
    pl.semaphore_wait(barrier, count)

    def remote(src, dst, ssem, rsem, rr, tt):
        return pltpu.make_async_remote_copy(
            src_ref=src,
            dst_ref=dst,
            send_sem=ssem,
            recv_sem=rsem,
            device_id=(rr, tt),
            device_id_type=MESH_ID,
        )

    own_dn.wait()
    dn_sends = []
    for j in range(1, half_reps):
        dn_sends.append(
            remote(
                dn_b.at[r], dn_b.at[r], dn_ssem.at[j], dn_rsem.at[r],
                lax.rem(r + 2 * j, reps), t,
            )
        )
    dn_sends.append(
        remote(dn_b.at[r], dn_b.at[r], dn_fsem.at[0], dn_rsem.at[r], partner, t)
    )
    for c in dn_sends:
        c.start()
    own_v.wait()
    v_sends = [
        remote(
            vo_b, vf_b.at[slot], vf_ssem.at[j], vf_rsem.at[slot],
            lax.rem(r + 2 * j, reps), plane,
        )
        for j in range(half_reps)
    ]
    v_home = pltpu.make_async_copy(vo_b, vf_b.at[slot], vf_rsem.at[slot])
    for j in range(1, half_reps):
        v_sends[j].start()

    @pl.when(plane != t)
    def _():
        v_sends[0].start()

    @pl.when(plane == t)
    def _():
        v_home.start()

    hid.wait()

    @pl.loop(0, seqs // 16)
    def _(i):
        rows = pl.ds(pl.multiple_of(i * 16, 16), 16)
        x = hid_b[rows, :].astype(f32)
        square = jnp.mean(x * x, axis=-1, keepdims=True)
        norm_b[rows, :] = (
            x * lax.rsqrt(square + epsilon) * gain[...].astype(f32)
        ).astype(bf16)

    q_acc[...] = jnp.zeros_like(q_acc)
    kv_acc[...] = jnp.zeros_like(kv_acc)

    def project(lo, hi):
        @pl.loop(lo, hi)
        def _(i):
            for c in w_copies(i):
                c.wait()
            rows = pl.ds(pl.multiple_of(i * kc, kc), kc)
            x = norm_b[:, rows]
            q_acc[...] += nn_dot(x, wq_b[rows, :])
            for j in range(2):
                kv_acc[j] += nn_dot(x, wkv_b[j, rows, :])

    project(0, steps // 2)

    dn_fwd = []
    for j in range(half_reps - 1, 0, -1):
        src = lax.rem(r + 2 * j, reps)
        remote(dn_b.at[src], dn_b.at[src], dn_fsem.at[j], dn_rsem.at[src], partner, t).wait_recv()
        c = remote(dn_b.at[src], dn_b.at[src], dn_fsem.at[j], dn_rsem.at[src], partner, t)
        c.start()
        dn_fwd.append(c)
    for j in range(half_reps):
        src = lax.rem(partner + 2 * j, reps)
        remote(dn_b.at[src], dn_b.at[src], dn_fsem.at[j], dn_rsem.at[src], partner, t).wait_recv()

    part = jnp.zeros((seqs, 3 * rank), f32)
    for j in range(reps):
        start = (j * n + t) * block
        cols = pl.ds(pl.multiple_of(start // win * win, LANES), win)
        part = part + nt_dot(norm_b[:, cols], dn_b[j])
    inner_s[...] = part
    in_sends = []
    for j in range(1, n):
        c = remote(
            inner_s, inner_r.at[j], in_ssem.at[j], in_rsem.at[j], r, lax.rem(t + j, n)
        )
        c.start()
        in_sends.append(c)

    project(steps // 2, steps)

    v_fwd = []
    for i in range(groups):
        for z in range(n):
            s, _sr = source_of(i, z)
            pltpu.make_async_copy(vo_b, vf_b.at[s], vf_rsem.at[s]).wait()
            c = remote(
                vf_b.at[s], vf_b.at[s], vf_fsem.at[i * n + z], vf_rsem.at[s], partner, t
            )
            c.start()
            v_fwd.append(c)
    for i in range(groups):
        for z in range(n):
            s = n * (2 * i + 1 - core) + z
            pltpu.make_async_copy(vo_b, vf_b.at[s], vf_rsem.at[s]).wait()

    total = inner_s[...]
    for c in in_sends:
        c.wait_recv()
    for j in range(1, n):
        total = total + inner_r[j]
    inner = total.astype(bf16).astype(f32)
    lane = lax.broadcasted_iota(jnp.int32, (seqs, 2 * rank), 1)
    first = inner[:, : 2 * rank]
    inner_q = jnp.where(lane < rank, first, 0.0).astype(bf16)
    inner_k = jnp.where(lane < rank, 0.0, first).astype(bf16)
    inner_v = inner[:, 2 * rank :].astype(bf16)

    q_od = vf_b[:, :q_rows, :].reshape(reps * q_rows, 2 * rank)
    kv_up = (
        vf_b[:, q_rows + up_rows :, :]
        .astype(f32)
        .reshape(reps * kv_rows, 2 * rank)
        .astype(bf16)
    )
    q = q_acc[...] + adapter_scale * nt_dot(inner_q, q_od)
    nk = kv_acc[0] + adapter_scale * nt_dot(inner_k, kv_up)
    nv = kv_acc[1] + adapter_scale * nt_dot(inner_v, kv_up[:, :rank])

    cosv, sinv = cos[...], sin[...]

    def turn(x):
        return x * cosv + pltpu.roll(x, head_dim // 2, 1) * sinv

    for h in range(pad_heads):
        rows = pl.ds(h, seqs, stride=pad_heads)
        if h < heads:
            q3[rows, :] = turn(q[:, h * head_dim : (h + 1) * head_dim])
        else:
            q3[rows, :] = jnp.zeros((seqs, head_dim), f32)
    for j in range(kv_local):
        key = turn(nk[:, j * head_dim : (j + 1) * head_dim]).astype(bf16).astype(f32)
        val = nv[:, j * head_dim : (j + 1) * head_dim].astype(bf16).astype(f32)
        for g in range(pad_heads):
            if min(g // group, kv_local - 1) == j:
                rows = pl.ds(g, seqs, stride=pad_heads)
                nk3[rows, :] = key
                nv3[rows, :] = val

    cache = cache_k.shape[2]
    span = kv_local * cache
    score_scale = 1.0 / math.sqrt(head_dim)
    bs = 8
    per = ps // bs

    @pl.loop(0, seqs // bs)
    def _(i):
        @pl.when(lax.rem(i, per) == 0)
        def _():
            for c in cache_copies(i // per):
                c.wait()

        base = pl.multiple_of(i * (bs * pad_heads), bs * pad_heads)
        rows = pl.ds(base, bs * pad_heads)
        qq = q3[rows, :]
        hi = qq.astype(bf16).astype(f32)
        rest = qq - hi
        mid = rest.astype(bf16).astype(f32)
        low = rest - mid
        own = jnp.sum(qq * nk3[rows, :], axis=-1, keepdims=True) * score_scale
        row_id = lax.broadcasted_iota(jnp.int32, (pad_heads, span), 0)
        col_id = lax.broadcasted_iota(jnp.int32, (pad_heads, span), 1)
        mine = jnp.minimum(row_id // group, kv_local - 1) == col_id // cache
        pos = lax.rem(col_id, cache)
        for b in range(bs):
            sl = slice(b * pad_heads, (b + 1) * pad_heads)
            stack = jnp.concatenate([hi[sl], mid[sl], low[sl]], axis=0).astype(bf16)
            keys = k_b[i * bs + b].reshape(span, head_dim)
            dots = nt_dot(stack, keys)
            sc = (
                dots[:pad_heads]
                + dots[pad_heads : 2 * pad_heads]
                + dots[2 * pad_heads :]
            ) * score_scale
            live = jnp.logical_and(mine, pos < lengths[i * bs + b])
            top = jnp.maximum(
                jnp.max(jnp.where(live, sc, -1e30), axis=-1, keepdims=True), own[sl]
            )
            w = jnp.where(live, jnp.exp(sc - top), 0.0)
            ow = jnp.exp(own[sl] - top)
            denom = jnp.sum(w, axis=-1, keepdims=True) + ow
            probs = (w / denom).astype(bf16)
            own_p = (ow / denom).astype(bf16).astype(f32)
            vals = v_b[i * bs + b].reshape(span, head_dim)
            here = pl.ds(base + b * pad_heads, pad_heads)
            c3[here, :] = nn_dot(probs, vals) + own_p * nv3[here, :]

    for h in range(heads):
        ctx[:, h * head_dim : (h + 1) * head_dim] = c3[
            pl.ds(h, seqs, stride=pad_heads), :
        ].astype(bf16)

    mid_s[...] = nn_dot(ctx[...], q_od)
    mid_sends = []
    for j in range(1, n):
        c = remote(mid_s, mid_r.at[j], mid_ssem.at[j], mid_rsem.at[j], r, lax.rem(t + j, n))
        c.start()
        mid_sends.append(c)

    tile = min(512, half_w)
    offsets = []
    at = 0
    for _way, _half, hops in channels_of(n):
        offsets.append(at)
        at += hops
    rs_sends = []
    for ci, way, half, hops, k in sends:
        idx = ((way * k) % n) * 2 + half
        wo_copy(way * k, half).wait()
        place = offsets[ci] + k - 1
        if k < hops:
            remote(
                rs_s.at[place + 1], rs_r.at[place + 1], rs_ssem.at[place + 1],
                rs_rsem.at[place + 1], r, lax.rem(t + way + n, n),
            ).wait_recv()

        @pl.loop(0, half_w // tile)
        def _(i):
            cols = pl.ds(pl.multiple_of(i * tile, tile), tile)
            value = nn_dot(ctx[...], wo_b[idx, :, cols])
            if k < hops:
                value = value + rs_r[place + 1, :, cols].astype(f32)
            rs_s[place, :, cols] = value.astype(bf16)

        c = remote(
            rs_s.at[place], rs_r.at[place], rs_ssem.at[place], rs_rsem.at[place],
            r, lax.rem(t + way + n, n),
        )
        c.start()
        rs_sends.append((c, k))

    total_mid = mid_s[:, rank:]
    for c in mid_sends:
        c.wait_recv()
    for j in range(1, n):
        total_mid = total_mid + mid_r[j][:, rank:]
    middle = total_mid.astype(bf16)
    ups = vf_b[:, q_rows : q_rows + up_rows, :].astype(f32)
    up_full = (
        jnp.concatenate([ups[:, :, :rank], ups[:, :, rank:]], axis=1)
        .reshape(reps * 2 * up_rows, rank)
        .astype(bf16)
    )
    final = []
    for half in range(2):
        wo_copy(0, half).wait()
        final.append(
            nn_dot(ctx[...], wo_b[half])
            + adapter_scale * nt_dot(middle, up_full[half * half_w : (half + 1) * half_w])
        )
    for c, k in rs_sends:
        if k == 1:
            c.wait_recv()
    for half in range(2):
        value = final[half]
        for ci, (_way, h2, hops) in enumerate(channels_of(n)):
            if h2 == half and hops > 0:
                value = value + rs_r[offsets[ci]].astype(f32)
        out[:, half * half_w : (half + 1) * half_w] = value.astype(bf16)

    for c in dn_sends + dn_fwd + v_fwd + in_sends + mid_sends:
        c.wait_send()
    for j in range(1, half_reps):
        v_sends[j].wait_send()

    @pl.when(plane != t)
    def _():
        v_sends[0].wait_send()

    for c, _k in rs_sends:
        c.wait_send()


def local(
    hidden,
    norm_gain,
    query_weight_matrix,
    key_value_weight,
    output_weight_matrix,
    input_down_factors,
    query_up_factor,
    key_value_up_factors,
    output_down_factor,
    output_up_factor,
    cache_keys,
    cache_values,
    lengths,
):
    reps, n = lax.axis_size("rep"), lax.axis_size("tp")
    r, t = lax.axis_index("rep"), lax.axis_index("tp")
    seqs, depth = hidden.shape
    _, kv_local, cache, head_dim = cache_keys.shape
    width = query_weight_matrix.shape[1]
    heads = width // head_dim
    rank = input_down_factors.shape[2]
    block = input_down_factors.shape[1]
    win = max(block, LANES)

    down = jnp.swapaxes(input_down_factors, 1, 2).reshape(3 * rank, block)
    if win != block:
        spot = lax.rem((r * n + t) * block, win)
        down = lax.dynamic_update_slice(
            jnp.zeros((3 * rank, win), down.dtype), down, (0, spot)
        )
    q_rows = query_up_factor.shape[1]
    kv_rows = key_value_up_factors.shape[2]
    up = output_up_factor.T
    up_rows = up.shape[0] // 2
    packed = jnp.concatenate(
        [
            jnp.concatenate([query_up_factor.T, output_down_factor], axis=1),
            jnp.concatenate([up[:up_rows], up[up_rows:]], axis=1),
            jnp.concatenate([key_value_up_factors[1].T, key_value_up_factors[0].T], axis=1),
        ],
        axis=0,
    )
    half_dim = head_dim // 2
    frequency = rope_base ** (-(jnp.arange(half_dim, dtype=f32) * 2.0) / head_dim)
    angles = lengths.astype(f32)[:, None] * frequency[None, :]
    cosine, sine = jnp.cos(angles), jnp.sin(angles)
    cos2 = jnp.concatenate([cosine, cosine], axis=1)
    sin2 = jnp.concatenate([-sine, sine], axis=1)

    dims = dict(
        tp=n, rep=reps, rank=rank, block=block, win=win,
        q_rows=q_rows, up_rows=up_rows, kv_rows=kv_rows,
    )
    pad_heads = -(-heads // 8) * 8
    wide = depth // n
    half_w = wide // 2
    rows = seqs * pad_heads
    slots = sum(hops for _, _, hops in channels_of(n))
    steps, parts = 16, 4
    dma = pltpu.SemaphoreType.DMA
    hbm = pl.BlockSpec(memory_space=pl.ANY)
    vmem = pl.BlockSpec(memory_space=pltpu.VMEM)
    smem = pl.BlockSpec(memory_space=pltpu.SMEM)
    vec = pltpu.VMEM
    return pl.pallas_call(
        functools.partial(kernel, dims),
        name="decode_block",
        out_shape=jax.ShapeDtypeStruct((seqs, wide), bf16),
        in_specs=[hbm, vmem, hbm, hbm, hbm, hbm, hbm, hbm, hbm, smem, vmem, vmem],
        out_specs=vmem,
        scratch_shapes=[
            vec((seqs, depth), bf16),
            vec((seqs, depth), bf16),
            vec((depth, width), bf16),
            vec((2, depth, kv_local * head_dim), bf16),
            vec((2 * n, width, half_w), bf16),
            vec((seqs, kv_local, cache, head_dim), bf16),
            vec((seqs, kv_local, cache, head_dim), bf16),
            vec((reps, 3 * rank, win), bf16),
            vec(packed.shape, bf16),
            vec((reps,) + packed.shape, bf16),
            vec((seqs, width), f32),
            vec((2, seqs, kv_local * head_dim), f32),
            vec((seqs, 3 * rank), f32),
            vec((n, seqs, 3 * rank), f32),
            vec((rows, head_dim), f32),
            vec((rows, head_dim), f32),
            vec((rows, head_dim), f32),
            vec((rows, head_dim), f32),
            vec((seqs, width), bf16),
            vec((seqs, 2 * rank), f32),
            vec((n, seqs, 2 * rank), f32),
            vec((slots, seqs, half_w), bf16),
            vec((slots, seqs, half_w), bf16),
            dma,
            dma((steps,)),
            dma((steps,)),
            dma((2 * n,)),
            dma((parts,)),
            dma((parts,)),
            dma((2,)),
            dma((reps // 2,)),
            dma((reps,)),
            dma((reps // 2,)),
            dma((reps // 2,)),
            dma((reps,)),
            dma((reps // 2,)),
            dma((n,)),
            dma((n,)),
            dma((n,)),
            dma((n,)),
            dma((slots,)),
            dma((slots,)),
        ],
        compiler_params=pltpu.CompilerParams(
            collective_id=0, has_side_effects=True, vmem_limit_bytes=66000000
        ),
    )(
        hidden,
        norm_gain.reshape(1, -1),
        query_weight_matrix,
        key_value_weight,
        output_weight_matrix,
        down,
        packed,
        cache_keys,
        cache_values,
        lengths,
        cos2,
        sin2,
    )


def solution(mesh):
    return jax.shard_map(
        local,
        mesh=mesh,
        in_specs=(
            P("rep", None),
            P(),
            P(None, "tp"),
            P(None, None, "tp"),
            P("tp", None),
            P(None, ("rep", "tp"), None),
            P(None, ("rep", "tp")),
            P(None, None, ("rep", "tp")),
            P(("rep", "tp"), None),
            P(None, ("rep", "tp")),
            P("rep", "tp", None, None),
            P("rep", "tp", None, None),
            P("rep"),
        ),
        out_specs=P("rep", "tp"),
        check_vma=False,
    )
```

```python
import functools
import math

import jax
import jax.numpy as jnp
from jax import lax
from jax.experimental import pallas as pl
from jax.experimental.pallas import tpu as pltpu
from jax.sharding import PartitionSpec as P

epsilon = 1e-06
rope_base = 1000000.0
adapter_scale = 0.5

f32 = jnp.float32
bf16 = jnp.bfloat16
LANES = 128
MESH_ID = pl.DeviceIdType.MESH


def nt_dot(left, right):
    return lax.dot_general(
        left, right, (((1,), (1,)), ((), ())), preferred_element_type=f32
    )


def nn_dot(left, right):
    return jnp.dot(left, right, preferred_element_type=f32)


def channels_of(n):
    return ((1, 0, n // 2), (-1, 1, n // 2), (1, 1, n // 2 - 1), (-1, 0, n // 2 - 1))


def kernel(
    dims,
    hidden,
    gain,
    wq,
    wkv,
    wo,
    dn_own,
    f_q,
    f_kv,
    f_od,
    f_ou,
    cache_k,
    cache_v,
    lengths,
    out,
    hid_b,
    norm_b,
    wq_b,
    wkv_b,
    wo_b,
    k_b,
    v_b,
    dn_b,
    a_q,
    a_kv,
    a_od,
    a_ou,
    g_q,
    g_kv,
    g_od,
    g_ou,
    angle,
    q_acc,
    kv_acc,
    inner_s,
    inner_r,
    q3,
    nk3,
    nv3,
    c3,
    ctx,
    mid_s,
    mid_r,
    rs_s,
    rs_r,
    hid_sem,
    w_sem,
    kv_sem,
    wo_sem,
    k_sem,
    v_sem,
    own_sem,
    dn_ssem,
    dn_rsem,
    dn_fsem,
    a_ssem,
    a_rsem,
    g_ssem,
    g_rsem,
    g_fsem,
    in_ssem,
    in_rsem,
    mid_ssem,
    mid_rsem,
    rs_ssem,
    rs_rsem,
):
    n, reps = dims["tp"], dims["rep"]
    seqs, depth = hidden.shape
    head_dim = cache_k.shape[3]
    kv_local = cache_k.shape[1]
    heads = wq.shape[1] // head_dim
    group = heads // kv_local
    pad_heads = q3.shape[0] // seqs
    rank = dims["rank"]
    block, win = dims["block"], dims["win"]
    half_reps = reps // 2
    r = lax.axis_index("rep")
    t = lax.axis_index("tp")
    core = lax.rem(r, 2)
    partner = r + 1 - 2 * core

    own_dn = pltpu.make_async_copy(dn_own, dn_b.at[r], own_sem.at[0])
    mine_at = r // 2
    spread = (a_q, a_kv, a_od, a_ou)
    gathered = (g_q, g_kv, g_od, g_ou)
    own_f = [
        pltpu.make_async_copy(src, dst.at[mine_at], own_sem.at[1 + f])
        for f, (src, dst) in enumerate(zip((f_q, f_kv, f_od, f_ou), spread))
    ]
    own_dn.start()
    for c in own_f:
        c.start()
    hid = pltpu.make_async_copy(hidden, hid_b, hid_sem)
    hid.start()
    steps = w_sem.shape[0]
    kc = depth // steps

    def w_copies(i):
        rows = pl.ds(pl.multiple_of(i * kc, kc), kc)
        return (
            pltpu.make_async_copy(wq.at[rows, :], wq_b.at[rows, :], w_sem.at[i]),
            pltpu.make_async_copy(wkv.at[:, rows, :], wkv_b.at[:, rows, :], kv_sem.at[i]),
        )

    @pl.loop(0, steps)
    def _(i):
        for c in w_copies(i):
            c.start()

    parts = k_sem.shape[0]
    ps = seqs // parts

    def cache_copies(i):
        rows = pl.ds(i * ps, ps)
        return (
            pltpu.make_async_copy(cache_k.at[rows], k_b.at[rows], k_sem.at[i]),
            pltpu.make_async_copy(cache_v.at[rows], v_b.at[rows], v_sem.at[i]),
        )

    @pl.loop(0, parts)
    def _(i):
        for c in cache_copies(i):
            c.start()

    wide = wo.shape[1] // n
    half_w = wide // 2

    def out_cols(k, half):
        d = lax.rem(t + k + n, n)
        return pl.ds(pl.multiple_of(d * wide + half * half_w, LANES), half_w)

    def wo_copy(k, half):
        cols = out_cols(k, half)
        idx = (k % n) * 2 + half
        return pltpu.make_async_copy(wo.at[:, cols], wo_b.at[idx], wo_sem.at[idx])

    sends = []
    for k in range(n // 2, 0, -1):
        for fresh in (True, False):
            for ci, (way, half, hops) in enumerate(channels_of(n)):
                if k <= hops and (k == hops) == fresh:
                    sends.append((ci, way, half, hops, k))
    for _ci, way, half, _hops, k in sends:
        wo_copy(way * k, half).start()
    wo_copy(0, 0).start()
    wo_copy(0, 1).start()

    barrier = pltpu.get_barrier_semaphore()

    def greet(rr, tt):
        pl.semaphore_signal(barrier, inc=1, device_id=(rr, tt), device_id_type=MESH_ID)

    count = 0
    greet(partner, t)
    count += 1
    for j in range(1, n):
        greet(r, lax.rem(t + j, n))
        count += 1
    for j in range(1, half_reps):
        greet(lax.rem(r + 2 * j, reps), t)
        count += 1

    pl.semaphore_wait(barrier, count)

    def remote(src, dst, ssem, rsem, rr, tt):
        return pltpu.make_async_remote_copy(
            src_ref=src,
            dst_ref=dst,
            send_sem=ssem,
            recv_sem=rsem,
            device_id=(rr, tt),
            device_id_type=MESH_ID,
        )

    own_dn.wait()
    dn_sends = []
    for j in range(1, half_reps):
        dn_sends.append(
            remote(
                dn_b.at[r], dn_b.at[r], dn_ssem.at[j], dn_rsem.at[r],
                lax.rem(r + 2 * j, reps), t,
            )
        )
    dn_sends.append(
        remote(dn_b.at[r], dn_b.at[r], dn_fsem.at[0], dn_rsem.at[r], partner, t)
    )
    for c in dn_sends:
        c.start()
    a_sends = []
    for f, buf in enumerate(spread):
        own_f[f].wait()
        for j in range(1, half_reps):
            c = remote(
                buf.at[mine_at], buf.at[mine_at], a_ssem.at[f, j], a_rsem.at[f, mine_at],
                lax.rem(r + 2 * j, reps), t,
            )
            c.start()
            a_sends.append(c)

    per_plane = reps // n
    groups = per_plane // 2
    g_sends = []

    def to_planes(f):
        buf, full = spread[f], gathered[f]
        for j in range(1, half_reps):
            src = lax.rem(r + 2 * j, reps) // 2
            remote(
                buf.at[src], buf.at[src], a_ssem.at[f, j], a_rsem.at[f, src], r, t
            ).wait_recv()
        for i in range(groups):
            s = n * (2 * i + core) + t
            for j in range(1, n):
                plane = lax.rem(t + j, n)
                src = (plane * per_plane + 2 * i) // 2
                c = remote(
                    buf.at[src], full.at[s], g_ssem.at[f, i * n + j], g_rsem.at[f, s],
                    r, plane,
                )
                c.start()
                g_sends.append(c)
            src = (t * per_plane + 2 * i) // 2
            pltpu.make_async_copy(buf.at[src], full.at[s], g_rsem.at[f, s]).start()

    def across(f):
        full = gathered[f]
        for i in range(groups):
            for z in range(n):
                s = n * (2 * i + core) + z
                pltpu.make_async_copy(spread[f].at[0], full.at[s], g_rsem.at[f, s]).wait()
                c = remote(
                    full.at[s], full.at[s], g_fsem.at[f, i * n + z], g_rsem.at[f, s],
                    partner, t,
                )
                c.start()
                g_sends.append(c)

    def settled(f):
        full = gathered[f]
        for i in range(groups):
            for z in range(n):
                s = n * (2 * i + 1 - core) + z
                pltpu.make_async_copy(spread[f].at[0], full.at[s], g_rsem.at[f, s]).wait()

    half_dim = head_dim // 2
    step = lax.rem(lax.broadcasted_iota(jnp.int32, (1, head_dim), 1), half_dim)
    frequency = jnp.exp(step.astype(f32) * (-2.0 * math.log(rope_base) / head_dim))

    @pl.loop(0, seqs // 8)
    def _(i):
        for b in range(8):
            angle[pl.ds(i * 8 + b, 1), :] = lengths[i * 8 + b].astype(f32) * frequency

    hid.wait()

    @pl.loop(0, seqs // 16)
    def _(i):
        rows = pl.ds(pl.multiple_of(i * 16, 16), 16)
        x = hid_b[rows, :].astype(f32)
        square = jnp.mean(x * x, axis=-1, keepdims=True)
        norm_b[rows, :] = (
            x * lax.rsqrt(square + epsilon) * gain[...].astype(f32)
        ).astype(bf16)

    q_acc[...] = jnp.zeros_like(q_acc)
    kv_acc[...] = jnp.zeros_like(kv_acc)

    def project(lo, hi):
        @pl.loop(lo, hi)
        def _(i):
            for c in w_copies(i):
                c.wait()
            rows = pl.ds(pl.multiple_of(i * kc, kc), kc)
            x = norm_b[:, rows]
            q_acc[...] += nn_dot(x, wq_b[rows, :])
            for j in range(2):
                kv_acc[j] += nn_dot(x, wkv_b[j, rows, :])

    project(0, steps // 4)
    to_planes(0)
    to_planes(1)
    project(steps // 4, steps // 2)

    dn_fwd = []
    for j in range(half_reps - 1, 0, -1):
        src = lax.rem(r + 2 * j, reps)
        remote(dn_b.at[src], dn_b.at[src], dn_fsem.at[j], dn_rsem.at[src], partner, t).wait_recv()
        c = remote(dn_b.at[src], dn_b.at[src], dn_fsem.at[j], dn_rsem.at[src], partner, t)
        c.start()
        dn_fwd.append(c)
    for j in range(half_reps):
        src = lax.rem(partner + 2 * j, reps)
        remote(dn_b.at[src], dn_b.at[src], dn_fsem.at[j], dn_rsem.at[src], partner, t).wait_recv()

    part = jnp.zeros((seqs, 3 * rank), f32)
    for j in range(reps):
        start = (j * n + t) * block
        cols = pl.ds(pl.multiple_of(start // win * win, LANES), win)
        part = part + nt_dot(norm_b[:, cols], dn_b[j])
    inner_s[...] = part
    in_sends = []
    for j in range(1, n):
        c = remote(
            inner_s, inner_r.at[j], in_ssem.at[j], in_rsem.at[j], r, lax.rem(t + j, n)
        )
        c.start()
        in_sends.append(c)

    across(0)
    across(1)
    to_planes(2)
    to_planes(3)
    project(steps // 2, steps)
    settled(0)
    settled(1)

    total = inner_s[...]
    for c in in_sends:
        c.wait_recv()
    for j in range(1, n):
        total = total + inner_r[j]
    inner = total.astype(bf16).astype(f32)
    inner_q = inner[:, :rank].astype(bf16)
    inner_k = inner[:, rank : 2 * rank].astype(bf16)
    inner_v = inner[:, 2 * rank :].astype(bf16)

    def rows_of(j):
        w = g_kv.shape[2]
        return g_kv[:, j].astype(f32).reshape(reps * w, rank).astype(bf16)

    q_up = jnp.concatenate([g_q[s] for s in range(reps)], axis=1)
    q = q_acc[...] + adapter_scale * nn_dot(inner_q, q_up)
    nk = kv_acc[0] + adapter_scale * nt_dot(inner_k, rows_of(0))
    nv = kv_acc[1] + adapter_scale * nt_dot(inner_v, rows_of(1))

    across(2)
    across(3)

    cosv = jnp.cos(angle[...])
    sinv = jnp.sin(angle[...])
    lane = lax.broadcasted_iota(jnp.int32, (seqs, head_dim), 1)
    sinv = jnp.where(lane < half_dim, -sinv, sinv)

    def turn(x):
        return x * cosv + pltpu.roll(x, head_dim // 2, 1) * sinv

    for h in range(pad_heads):
        rows = pl.ds(h, seqs, stride=pad_heads)
        if h < heads:
            q3[rows, :] = turn(q[:, h * head_dim : (h + 1) * head_dim])
        else:
            q3[rows, :] = jnp.zeros((seqs, head_dim), f32)
    for j in range(kv_local):
        key = turn(nk[:, j * head_dim : (j + 1) * head_dim]).astype(bf16).astype(f32)
        val = nv[:, j * head_dim : (j + 1) * head_dim].astype(bf16).astype(f32)
        for g in range(pad_heads):
            if min(g // group, kv_local - 1) == j:
                rows = pl.ds(g, seqs, stride=pad_heads)
                nk3[rows, :] = key
                nv3[rows, :] = val

    cache = cache_k.shape[2]
    span = kv_local * cache
    score_scale = 1.0 / math.sqrt(head_dim)
    bs = min(16, ps)
    per = ps // bs

    @pl.loop(0, seqs // bs)
    def _(i):
        @pl.when(lax.rem(i, per) == 0)
        def _():
            for c in cache_copies(i // per):
                c.wait()

        base = pl.multiple_of(i * (bs * pad_heads), bs * pad_heads)
        rows = pl.ds(base, bs * pad_heads)
        qq = q3[rows, :]
        hi = qq.astype(bf16).astype(f32)
        rest = qq - hi
        mid = rest.astype(bf16).astype(f32)
        low = rest - mid
        own = jnp.sum(qq * nk3[rows, :], axis=-1, keepdims=True) * score_scale
        row_id = lax.broadcasted_iota(jnp.int32, (pad_heads, span), 0)
        col_id = lax.broadcasted_iota(jnp.int32, (pad_heads, span), 1)
        mine = jnp.minimum(row_id // group, kv_local - 1) == col_id // cache
        pos = lax.rem(col_id, cache)
        scored = []
        for b in range(bs):
            sl = slice(b * pad_heads, (b + 1) * pad_heads)
            stack = jnp.concatenate([hi[sl], mid[sl], low[sl]], axis=0).astype(bf16)
            keys = k_b[i * bs + b].reshape(span, head_dim)
            dots = nt_dot(stack, keys)
            sc = (
                dots[:pad_heads]
                + dots[pad_heads : 2 * pad_heads]
                + dots[2 * pad_heads :]
            ) * score_scale
            live = jnp.logical_and(mine, pos < lengths[i * bs + b])
            scored.append(jnp.where(live, sc, -1e30))
        sc = jnp.concatenate(scored, axis=0)
        top = jnp.maximum(jnp.max(sc, axis=-1, keepdims=True), own)
        w = jnp.exp(sc - top)
        ow = jnp.exp(own - top)
        scale = 1.0 / (jnp.sum(w, axis=-1, keepdims=True) + ow)
        probs = w * scale
        own_part = (ow * scale).astype(bf16).astype(f32) * nv3[rows, :]
        for b in range(bs):
            sl = slice(b * pad_heads, (b + 1) * pad_heads)
            vals = v_b[i * bs + b].reshape(span, head_dim)
            here = pl.ds(base + b * pad_heads, pad_heads)
            c3[here, :] = nn_dot(probs[sl].astype(bf16), vals) + own_part[sl]

    for h in range(heads):
        ctx[:, h * head_dim : (h + 1) * head_dim] = c3[
            pl.ds(h, seqs, stride=pad_heads), :
        ].astype(bf16)

    settled(2)
    settled(3)
    down_t = jnp.concatenate([g_od[s] for s in range(reps)], axis=1)
    mid_s[...] = nt_dot(ctx[...], down_t)
    mid_sends = []
    for j in range(1, n):
        c = remote(mid_s, mid_r.at[j], mid_ssem.at[j], mid_rsem.at[j], r, lax.rem(t + j, n))
        c.start()
        mid_sends.append(c)

    tile = min(512, half_w)
    offsets = []
    at = 0
    for _way, _half, hops in channels_of(n):
        offsets.append(at)
        at += hops
    rs_sends = []
    for ci, way, half, hops, k in sends:
        idx = ((way * k) % n) * 2 + half
        wo_copy(way * k, half).wait()
        place = offsets[ci] + k - 1
        if k < hops:
            remote(
                rs_s.at[place + 1], rs_r.at[place + 1], rs_ssem.at[place + 1],
                rs_rsem.at[place + 1], r, lax.rem(t + way + n, n),
            ).wait_recv()

        @pl.loop(0, half_w // tile)
        def _(i):
            cols = pl.ds(pl.multiple_of(i * tile, tile), tile)
            value = nn_dot(ctx[...], wo_b[idx, :, cols])
            if k < hops:
                value = value + rs_r[place + 1, :, cols].astype(f32)
            rs_s[place, :, cols] = value.astype(bf16)

        c = remote(
            rs_s.at[place], rs_r.at[place], rs_ssem.at[place], rs_rsem.at[place],
            r, lax.rem(t + way + n, n),
        )
        c.start()
        rs_sends.append((c, k))

    total_mid = mid_s[...]
    for c in mid_sends:
        c.wait_recv()
    for j in range(1, n):
        total_mid = total_mid + mid_r[j]
    middle = total_mid.astype(bf16)
    up_full = jnp.concatenate([g_ou[s] for s in range(reps)], axis=1)
    final = []
    for half in range(2):
        wo_copy(0, half).wait()
        final.append(
            nn_dot(ctx[...], wo_b[half])
            + adapter_scale * nn_dot(middle, up_full[:, half * half_w : (half + 1) * half_w])
        )
    for c, k in rs_sends:
        if k == 1:
            c.wait_recv()
    for half in range(2):
        value = final[half]
        for ci, (_way, h2, hops) in enumerate(channels_of(n)):
            if h2 == half and hops > 0:
                value = value + rs_r[offsets[ci]].astype(f32)
        out[:, half * half_w : (half + 1) * half_w] = value.astype(bf16)

    for c in dn_sends + dn_fwd + a_sends + g_sends + in_sends + mid_sends:
        c.wait_send()
    for c, _k in rs_sends:
        c.wait_send()


def local(
    hidden,
    norm_gain,
    query_weight_matrix,
    key_value_weight,
    output_weight_matrix,
    input_down_factors,
    query_up_factor,
    key_value_up_factors,
    output_down_factor,
    output_up_factor,
    cache_keys,
    cache_values,
    lengths,
):
    reps, n = lax.axis_size("rep"), lax.axis_size("tp")
    r, t = lax.axis_index("rep"), lax.axis_index("tp")
    seqs, depth = hidden.shape
    _, kv_local, cache, head_dim = cache_keys.shape
    width = query_weight_matrix.shape[1]
    heads = width // head_dim
    rank = input_down_factors.shape[2]
    block = input_down_factors.shape[1]
    win = max(block, LANES)

    down = jnp.swapaxes(input_down_factors, 1, 2).reshape(3 * rank, block)
    if win != block:
        spot = lax.rem((r * n + t) * block, win)
        down = lax.dynamic_update_slice(
            jnp.zeros((3 * rank, win), down.dtype), down, (0, spot)
        )
    f_q = query_up_factor
    f_kv = jnp.swapaxes(key_value_up_factors, 1, 2)
    f_od = output_down_factor.T
    f_ou = output_up_factor
    factors = (f_q, f_kv, f_od, f_ou)
    dims = dict(
        tp=n, rep=reps, rank=rank, block=block, win=win,
    )
    pad_heads = -(-heads // 8) * 8
    wide = depth // n
    half_w = wide // 2
    rows = seqs * pad_heads
    slots = sum(hops for _, _, hops in channels_of(n))
    steps, parts = 16, 4
    dma = pltpu.SemaphoreType.DMA
    hbm = pl.BlockSpec(memory_space=pl.ANY)
    vmem = pl.BlockSpec(memory_space=pltpu.VMEM)
    smem = pl.BlockSpec(memory_space=pltpu.SMEM)
    vec = pltpu.VMEM
    return pl.pallas_call(
        functools.partial(kernel, dims),
        name="decode_block",
        out_shape=jax.ShapeDtypeStruct((seqs, wide), bf16),
        in_specs=[hbm, vmem] + [hbm] * 10 + [smem],
        out_specs=vmem,
        scratch_shapes=[
            vec((seqs, depth), bf16),
            vec((seqs, depth), bf16),
            vec((depth, width), bf16),
            vec((2, depth, kv_local * head_dim), bf16),
            vec((2 * n, width, half_w), bf16),
            vec((seqs, kv_local, cache, head_dim), bf16),
            vec((seqs, kv_local, cache, head_dim), bf16),
            vec((reps, 3 * rank, win), bf16),
            *[vec((reps // 2,) + f.shape, bf16) for f in factors],
            *[vec((reps,) + f.shape, bf16) for f in factors],
            vec((seqs, head_dim), f32),
            vec((seqs, width), f32),
            vec((2, seqs, kv_local * head_dim), f32),
            vec((seqs, 3 * rank), f32),
            vec((n, seqs, 3 * rank), f32),
            vec((rows, head_dim), f32),
            vec((rows, head_dim), f32),
            vec((rows, head_dim), f32),
            vec((rows, head_dim), f32),
            vec((seqs, width), bf16),
            vec((seqs, rank), f32),
            vec((n, seqs, rank), f32),
            vec((slots, seqs, half_w), bf16),
            vec((slots, seqs, half_w), bf16),
            dma,
            dma((steps,)),
            dma((steps,)),
            dma((2 * n,)),
            dma((parts,)),
            dma((parts,)),
            dma((1 + len(factors),)),
            dma((reps // 2,)),
            dma((reps,)),
            dma((reps // 2,)),
            dma((len(factors), reps // 2)),
            dma((len(factors), reps // 2)),
            dma((len(factors), reps)),
            dma((len(factors), reps)),
            dma((len(factors), reps)),
            dma((n,)),
            dma((n,)),
            dma((n,)),
            dma((n,)),
            dma((slots,)),
            dma((slots,)),
        ],
        compiler_params=pltpu.CompilerParams(
            collective_id=0, has_side_effects=True, vmem_limit_bytes=66000000
        ),
    )(
        hidden,
        norm_gain.reshape(1, -1),
        query_weight_matrix,
        key_value_weight,
        output_weight_matrix,
        down,
        *factors,
        cache_keys,
        cache_values,
        lengths,
    )


def solution(mesh):
    return jax.shard_map(
        local,
        mesh=mesh,
        in_specs=(
            P("rep", None),
            P(),
            P(None, "tp"),
            P(None, None, "tp"),
            P("tp", None),
            P(None, ("rep", "tp"), None),
            P(None, ("rep", "tp")),
            P(None, None, ("rep", "tp")),
            P(("rep", "tp"), None),
            P(None, ("rep", "tp")),
            P("rep", "tp", None, None),
            P("rep", "tp", None, None),
            P("rep"),
        ),
        out_specs=P("rep", "tp"),
        check_vma=False,
    )
```

```python
import functools
import math

import jax
import jax.numpy as jnp
from jax import lax
from jax.experimental import pallas as pl
from jax.experimental.pallas import tpu as pltpu
from jax.sharding import PartitionSpec as P

epsilon = 1e-06
rope_base = 1000000.0
adapter_scale = 0.5

f32 = jnp.float32
bf16 = jnp.bfloat16
LANES = 128
MESH_ID = pl.DeviceIdType.MESH


def nt_dot(left, right):
    return lax.dot_general(
        left, right, (((1,), (1,)), ((), ())), preferred_element_type=f32
    )


def nn_dot(left, right):
    return jnp.dot(left, right, preferred_element_type=f32)


def channels_of(n):
    return ((1, 0, n // 2), (-1, 1, n // 2), (1, 1, n // 2 - 1), (-1, 0, n // 2 - 1))


def kernel(
    dims,
    hidden,
    gain,
    wq,
    wkv,
    wo,
    dn_own,
    f_q,
    f_kv,
    f_od,
    f_ou,
    cache_k,
    cache_v,
    lengths,
    out,
    hid_b,
    norm_b,
    wq_b,
    wkv_b,
    wo_b,
    k_b,
    v_b,
    dn_b,
    a_q,
    a_kv,
    a_od,
    a_ou,
    g_q,
    g_kv,
    g_od,
    g_ou,
    angle,
    q_acc,
    kv_acc,
    inner_o,
    inner_s,
    inner_r,
    q3,
    nk3,
    nv3,
    c3,
    ctx,
    mid_s,
    mid_r,
    rs_s,
    rs_r,
    hid_sem,
    w_sem,
    kv_sem,
    wo_sem,
    k_sem,
    v_sem,
    own_sem,
    dn_ssem,
    dn_rsem,
    dn_fsem,
    a_ssem,
    a_rsem,
    g_ssem,
    g_rsem,
    g_fsem,
    in_ssem,
    in_rsem,
    mid_ssem,
    mid_rsem,
    rs_ssem,
    rs_rsem,
):
    n, reps = dims["tp"], dims["rep"]
    seqs, depth = hidden.shape
    head_dim = cache_k.shape[3]
    kv_local = cache_k.shape[1]
    heads = wq.shape[1] // head_dim
    group = heads // kv_local
    pad_heads = q3.shape[0] // seqs
    rank = dims["rank"]
    block, win = dims["block"], dims["win"]
    half_reps = reps // 2
    r = lax.axis_index("rep")
    t = lax.axis_index("tp")
    core = lax.rem(r, 2)
    partner = r + 1 - 2 * core

    own_dn = pltpu.make_async_copy(dn_own, dn_b.at[r], own_sem.at[0])
    mine_at = r // 2
    spread = (a_q, a_kv, a_od, a_ou)
    gathered = (g_q, g_kv, g_od, g_ou)
    own_f = [
        pltpu.make_async_copy(src, dst.at[mine_at], own_sem.at[1 + f])
        for f, (src, dst) in enumerate(zip((f_q, f_kv, f_od, f_ou), spread))
    ]
    own_dn.start()
    for c in own_f:
        c.start()
    hid = pltpu.make_async_copy(hidden, hid_b, hid_sem)
    hid.start()
    steps = w_sem.shape[0]
    kc = depth // steps

    def w_copies(i):
        rows = pl.ds(pl.multiple_of(i * kc, kc), kc)
        return (
            pltpu.make_async_copy(wq.at[rows, :], wq_b.at[rows, :], w_sem.at[i]),
            pltpu.make_async_copy(wkv.at[:, rows, :], wkv_b.at[:, rows, :], kv_sem.at[i]),
        )

    @pl.loop(0, steps)
    def _(i):
        for c in w_copies(i):
            c.start()

    parts = k_sem.shape[0]
    ps = seqs // parts

    def cache_copies(i):
        rows = pl.ds(i * ps, ps)
        return (
            pltpu.make_async_copy(cache_k.at[rows], k_b.at[rows], k_sem.at[i]),
            pltpu.make_async_copy(cache_v.at[rows], v_b.at[rows], v_sem.at[i]),
        )

    @pl.loop(0, parts)
    def _(i):
        for c in cache_copies(i):
            c.start()

    wide = wo.shape[1] // n
    half_w = wide // 2

    def out_cols(k, half):
        d = lax.rem(t + k + n, n)
        return pl.ds(pl.multiple_of(d * wide + half * half_w, LANES), half_w)

    def wo_copy(k, half):
        cols = out_cols(k, half)
        idx = (k % n) * 2 + half
        return pltpu.make_async_copy(wo.at[:, cols], wo_b.at[idx], wo_sem.at[idx])

    sends = []
    for k in range(n // 2, 0, -1):
        for fresh in (True, False):
            for ci, (way, half, hops) in enumerate(channels_of(n)):
                if k <= hops and (k == hops) == fresh:
                    sends.append((ci, way, half, hops, k))
    for _ci, way, half, _hops, k in sends:
        wo_copy(way * k, half).start()
    wo_copy(0, 0).start()
    wo_copy(0, 1).start()

    barrier = pltpu.get_barrier_semaphore()

    def greet(rr, tt):
        pl.semaphore_signal(barrier, inc=1, device_id=(rr, tt), device_id_type=MESH_ID)

    count = 0
    greet(partner, t)
    count += 1
    for j in range(1, n):
        greet(r, lax.rem(t + j, n))
        count += 1
    for j in range(1, half_reps):
        greet(lax.rem(r + 2 * j, reps), t)
        count += 1

    pl.semaphore_wait(barrier, count)

    def remote(src, dst, ssem, rsem, rr, tt):
        return pltpu.make_async_remote_copy(
            src_ref=src,
            dst_ref=dst,
            send_sem=ssem,
            recv_sem=rsem,
            device_id=(rr, tt),
            device_id_type=MESH_ID,
        )

    own_dn.wait()
    dn_sends = []
    for j in range(1, half_reps):
        dn_sends.append(
            remote(
                dn_b.at[r], dn_b.at[r], dn_ssem.at[j], dn_rsem.at[r],
                lax.rem(r + 2 * j, reps), t,
            )
        )
    dn_sends.append(
        remote(dn_b.at[r], dn_b.at[r], dn_fsem.at[0], dn_rsem.at[r], partner, t)
    )
    for c in dn_sends:
        c.start()
    a_sends = []

    def to_chips(f):
        buf = spread[f]
        own_f[f].wait()
        for j in range(1, half_reps):
            c = remote(
                buf.at[mine_at], buf.at[mine_at], a_ssem.at[f, j], a_rsem.at[f, mine_at],
                lax.rem(r + 2 * j, reps), t,
            )
            c.start()
            a_sends.append(c)

    to_chips(0)
    to_chips(1)
    per_plane = reps // n
    groups = per_plane // 2
    g_sends = []

    def to_planes(f):
        buf, full = spread[f], gathered[f]
        for j in range(1, half_reps):
            src = lax.rem(r + 2 * j, reps) // 2
            remote(
                buf.at[src], buf.at[src], a_ssem.at[f, j], a_rsem.at[f, src], r, t
            ).wait_recv()
        for i in range(groups):
            s = n * (2 * i + core) + t
            for j in range(1, n):
                plane = lax.rem(t + j, n)
                src = (plane * per_plane + 2 * i) // 2
                c = remote(
                    buf.at[src], full.at[s], g_ssem.at[f, i * n + j], g_rsem.at[f, s],
                    r, plane,
                )
                c.start()
                g_sends.append(c)
            src = (t * per_plane + 2 * i) // 2
            pltpu.make_async_copy(buf.at[src], full.at[s], g_rsem.at[f, s]).start()

    def across(f):
        full = gathered[f]
        for i in range(groups):
            for z in range(n):
                s = n * (2 * i + core) + z
                pltpu.make_async_copy(spread[f].at[0], full.at[s], g_rsem.at[f, s]).wait()
                c = remote(
                    full.at[s], full.at[s], g_fsem.at[f, i * n + z], g_rsem.at[f, s],
                    partner, t,
                )
                c.start()
                g_sends.append(c)

    def settled(f):
        full = gathered[f]
        for i in range(groups):
            for z in range(n):
                s = n * (2 * i + 1 - core) + z
                pltpu.make_async_copy(spread[f].at[0], full.at[s], g_rsem.at[f, s]).wait()

    half_dim = head_dim // 2
    step = lax.rem(lax.broadcasted_iota(jnp.int32, (1, head_dim), 1), half_dim)
    frequency = jnp.exp(step.astype(f32) * (-2.0 * math.log(rope_base) / head_dim))

    @pl.loop(0, seqs // 8)
    def _(i):
        for b in range(8):
            angle[pl.ds(i * 8 + b, 1), :] = lengths[i * 8 + b].astype(f32) * frequency

    hid.wait()

    @pl.loop(0, seqs // 16)
    def _(i):
        rows = pl.ds(pl.multiple_of(i * 16, 16), 16)
        x = hid_b[rows, :].astype(f32)
        square = jnp.mean(x * x, axis=-1, keepdims=True)
        norm_b[rows, :] = (
            x * lax.rsqrt(square + epsilon) * gain[...].astype(f32)
        ).astype(bf16)

    q_acc[...] = jnp.zeros_like(q_acc)
    kv_acc[...] = jnp.zeros_like(kv_acc)

    def project(lo, hi):
        @pl.loop(lo, hi)
        def _(i):
            for c in w_copies(i):
                c.wait()
            rows = pl.ds(pl.multiple_of(i * kc, kc), kc)
            x = norm_b[:, rows]
            q_acc[...] += nn_dot(x, wq_b[rows, :])
            for j in range(2):
                kv_acc[j] += nn_dot(x, wkv_b[j, rows, :])

    project(0, steps // 4)
    to_planes(0)
    to_planes(1)
    project(steps // 4, steps // 2)

    dn_fwd = []
    for j in range(half_reps - 1, 0, -1):
        src = lax.rem(r + 2 * j, reps)
        remote(dn_b.at[src], dn_b.at[src], dn_fsem.at[j], dn_rsem.at[src], partner, t).wait_recv()
        c = remote(dn_b.at[src], dn_b.at[src], dn_fsem.at[j], dn_rsem.at[src], partner, t)
        c.start()
        dn_fwd.append(c)
    for j in range(half_reps):
        src = lax.rem(partner + 2 * j, reps)
        remote(dn_b.at[src], dn_b.at[src], dn_fsem.at[j], dn_rsem.at[src], partner, t).wait_recv()

    part = jnp.zeros((seqs, 3 * rank), f32)
    for j in range(reps):
        start = (j * n + t) * block
        cols = pl.ds(pl.multiple_of(start // win * win, LANES), win)
        part = part + nt_dot(norm_b[:, cols], dn_b[j])
    inner_s[...] = part.astype(bf16)
    inner_o[...] = part
    in_sends = []
    for j in range(1, n):
        c = remote(
            inner_s, inner_r.at[j], in_ssem.at[j], in_rsem.at[j], r, lax.rem(t + j, n)
        )
        c.start()
        in_sends.append(c)

    across(0)
    across(1)
    to_chips(2)
    to_chips(3)
    project(steps // 2, 3 * steps // 4)
    to_planes(2)
    to_planes(3)
    project(3 * steps // 4, steps)
    settled(0)
    settled(1)

    total = inner_o[...]
    for c in in_sends:
        c.wait_recv()
    for j in range(1, n):
        total = total + inner_r[j].astype(f32)
    inner = total.astype(bf16).astype(f32)
    inner_q = inner[:, :rank].astype(bf16)
    inner_k = inner[:, rank : 2 * rank].astype(bf16)
    inner_v = inner[:, 2 * rank :].astype(bf16)

    def rows_of(j):
        w = g_kv.shape[2]
        return g_kv[:, j].astype(f32).reshape(reps * w, rank).astype(bf16)

    q_up = jnp.concatenate([g_q[s] for s in range(reps)], axis=1)
    q = q_acc[...] + adapter_scale * nn_dot(inner_q, q_up)
    nk = kv_acc[0] + adapter_scale * nt_dot(inner_k, rows_of(0))
    nv = kv_acc[1] + adapter_scale * nt_dot(inner_v, rows_of(1))

    across(2)
    across(3)

    cosv = jnp.cos(angle[...])
    sinv = jnp.sin(angle[...])
    lane = lax.broadcasted_iota(jnp.int32, (seqs, head_dim), 1)
    sinv = jnp.where(lane < half_dim, -sinv, sinv)

    def turn(x):
        return x * cosv + pltpu.roll(x, head_dim // 2, 1) * sinv

    for h in range(pad_heads):
        rows = pl.ds(h, seqs, stride=pad_heads)
        if h < heads:
            q3[rows, :] = turn(q[:, h * head_dim : (h + 1) * head_dim])
        else:
            q3[rows, :] = jnp.zeros((seqs, head_dim), f32)
    for j in range(kv_local):
        key = turn(nk[:, j * head_dim : (j + 1) * head_dim]).astype(bf16).astype(f32)
        val = nv[:, j * head_dim : (j + 1) * head_dim].astype(bf16).astype(f32)
        for g in range(pad_heads):
            if min(g // group, kv_local - 1) == j:
                rows = pl.ds(g, seqs, stride=pad_heads)
                nk3[rows, :] = key
                nv3[rows, :] = val

    cache = cache_k.shape[2]
    span = kv_local * cache
    score_scale = 1.0 / math.sqrt(head_dim)
    bs = min(16, ps)
    per = ps // bs

    def attend(i):
        @pl.when(lax.rem(i, per) == 0)
        def _():
            for c in cache_copies(i // per):
                c.wait()

        base = pl.multiple_of(i * (bs * pad_heads), bs * pad_heads)
        rows = pl.ds(base, bs * pad_heads)
        qq = q3[rows, :]
        hi = qq.astype(bf16).astype(f32)
        rest = qq - hi
        mid = rest.astype(bf16).astype(f32)
        low = rest - mid
        own = jnp.sum(qq * nk3[rows, :], axis=-1, keepdims=True) * score_scale
        row_id = lax.broadcasted_iota(jnp.int32, (pad_heads, span), 0)
        col_id = lax.broadcasted_iota(jnp.int32, (pad_heads, span), 1)
        mine = jnp.minimum(row_id // group, kv_local - 1) == col_id // cache
        pos = lax.rem(col_id, cache)
        scored = []
        for b in range(bs):
            sl = slice(b * pad_heads, (b + 1) * pad_heads)
            stack = jnp.concatenate([hi[sl], mid[sl], low[sl]], axis=0).astype(bf16)
            keys = k_b[i * bs + b].reshape(span, head_dim)
            dots = nt_dot(stack, keys)
            sc = (
                dots[:pad_heads]
                + dots[pad_heads : 2 * pad_heads]
                + dots[2 * pad_heads :]
            ) * score_scale
            live = jnp.logical_and(mine, pos < lengths[i * bs + b])
            scored.append(jnp.where(live, sc, -1e30))
        sc = jnp.concatenate(scored, axis=0)
        top = jnp.maximum(jnp.max(sc, axis=-1, keepdims=True), own)
        w = jnp.exp(sc - top)
        ow = jnp.exp(own - top)
        scale = 1.0 / (jnp.sum(w, axis=-1, keepdims=True) + ow)
        probs = w * scale
        own_part = (ow * scale).astype(bf16).astype(f32) * nv3[rows, :]
        for b in range(bs):
            sl = slice(b * pad_heads, (b + 1) * pad_heads)
            vals = v_b[i * bs + b].reshape(span, head_dim)
            here = pl.ds(base + b * pad_heads, pad_heads)
            c3[here, :] = nn_dot(probs[sl].astype(bf16), vals) + own_part[sl]

    waves = rs_s.shape[0]
    ws = seqs // waves

    def attend_wave(wave):
        pl.loop(wave * ws // bs, (wave + 1) * ws // bs)(attend)
        for h in range(heads):
            ctx[wave * ws : (wave + 1) * ws, h * head_dim : (h + 1) * head_dim] = c3[
                pl.ds(wave * ws * pad_heads + h, ws, stride=pad_heads), :
            ].astype(bf16)

    tile = min(512, half_w)
    offsets = []
    at = 0
    for _way, _half, hops in channels_of(n):
        offsets.append(at)
        at += hops
    rs_sends = []

    def hop(wave, place, way):
        return remote(
            rs_s.at[wave, place], rs_r.at[wave, place], rs_ssem.at[wave, place],
            rs_rsem.at[wave, place], r, lax.rem(t + way + n, n),
        )

    def pass_on(wave, ci, way, half, hops, k):
        idx = ((way * k) % n) * 2 + half
        place = offsets[ci] + k - 1
        if wave == 0:
            wo_copy(way * k, half).wait()
        if k < hops:
            hop(wave, place + 1, way).wait_recv()

        @pl.loop(0, half_w // tile)
        def _(i):
            cols = pl.ds(pl.multiple_of(i * tile, tile), tile)
            value = nn_dot(ctx[wave * ws : (wave + 1) * ws, :], wo_b[idx, :, cols])
            if k < hops:
                value = value + rs_r[wave, place + 1, :, cols].astype(f32)
            rs_s[wave, place, :, cols] = value.astype(bf16)

        c = hop(wave, place, way)
        c.start()
        rs_sends.append((c, k))

    early = [x for x in sends if x[3] == x[4] == n // 2]
    lone = [x for x in sends if x[3] == x[4] != n // 2]
    joined = [x for x in sends if x[3] != x[4]]
    attend_wave(0)
    for x in early + lone:
        pass_on(0, *x)
    for wave in range(1, waves):
        attend_wave(wave)
        for x in early:
            pass_on(wave, *x)
        for x in joined:
            pass_on(wave - 1, *x)
        for x in lone:
            pass_on(wave, *x)

    settled(2)
    settled(3)
    down_t = jnp.concatenate([g_od[s] for s in range(reps)], axis=1)
    total_mid = nt_dot(ctx[...], down_t)
    mid_s[...] = total_mid.astype(bf16)
    mid_sends = []
    for j in range(1, n):
        c = remote(mid_s, mid_r.at[j], mid_ssem.at[j], mid_rsem.at[j], r, lax.rem(t + j, n))
        c.start()
        mid_sends.append(c)
    for x in joined:
        pass_on(waves - 1, *x)

    for c in mid_sends:
        c.wait_recv()
    for j in range(1, n):
        total_mid = total_mid + mid_r[j].astype(f32)
    middle = total_mid.astype(bf16)
    up_full = jnp.concatenate([g_ou[s] for s in range(reps)], axis=1)
    final = []
    for half in range(2):
        wo_copy(0, half).wait()
        final.append(
            nn_dot(ctx[...], wo_b[half])
            + adapter_scale * nn_dot(middle, up_full[:, half * half_w : (half + 1) * half_w])
        )
    for c, k in rs_sends:
        if k == 1:
            c.wait_recv()
    for half in range(2):
        value = final[half]
        for ci, (_way, h2, hops) in enumerate(channels_of(n)):
            if h2 == half and hops > 0:
                value = value + rs_r[:, offsets[ci]].reshape(seqs, half_w).astype(f32)
        out[:, half * half_w : (half + 1) * half_w] = value.astype(bf16)

    for c in dn_sends + dn_fwd + a_sends + g_sends + in_sends + mid_sends:
        c.wait_send()
    for c, _k in rs_sends:
        c.wait_send()


def local(
    hidden,
    norm_gain,
    query_weight_matrix,
    key_value_weight,
    output_weight_matrix,
    input_down_factors,
    query_up_factor,
    key_value_up_factors,
    output_down_factor,
    output_up_factor,
    cache_keys,
    cache_values,
    lengths,
):
    reps, n = lax.axis_size("rep"), lax.axis_size("tp")
    r, t = lax.axis_index("rep"), lax.axis_index("tp")
    seqs, depth = hidden.shape
    _, kv_local, cache, head_dim = cache_keys.shape
    width = query_weight_matrix.shape[1]
    heads = width // head_dim
    rank = input_down_factors.shape[2]
    block = input_down_factors.shape[1]
    win = max(block, LANES)

    down = jnp.swapaxes(input_down_factors, 1, 2).reshape(3 * rank, block)
    if win != block:
        spot = lax.rem((r * n + t) * block, win)
        down = lax.dynamic_update_slice(
            jnp.zeros((3 * rank, win), down.dtype), down, (0, spot)
        )
    f_q = query_up_factor
    f_kv = jnp.swapaxes(key_value_up_factors, 1, 2)
    f_od = output_down_factor.T
    f_ou = output_up_factor
    factors = (f_q, f_kv, f_od, f_ou)
    dims = dict(
        tp=n, rep=reps, rank=rank, block=block, win=win,
    )
    pad_heads = -(-heads // 8) * 8
    wide = depth // n
    half_w = wide // 2
    rows = seqs * pad_heads
    slots = sum(hops for _, _, hops in channels_of(n))
    steps, parts, waves = 16, 4, 2
    dma = pltpu.SemaphoreType.DMA
    hbm = pl.BlockSpec(memory_space=pl.ANY)
    vmem = pl.BlockSpec(memory_space=pltpu.VMEM)
    smem = pl.BlockSpec(memory_space=pltpu.SMEM)
    vec = pltpu.VMEM
    return pl.pallas_call(
        functools.partial(kernel, dims),
        name="decode_block",
        out_shape=jax.ShapeDtypeStruct((seqs, wide), bf16),
        in_specs=[hbm, vmem] + [hbm] * 10 + [smem],
        out_specs=vmem,
        scratch_shapes=[
            vec((seqs, depth), bf16),
            vec((seqs, depth), bf16),
            vec((depth, width), bf16),
            vec((2, depth, kv_local * head_dim), bf16),
            vec((2 * n, width, half_w), bf16),
            vec((seqs, kv_local, cache, head_dim), bf16),
            vec((seqs, kv_local, cache, head_dim), bf16),
            vec((reps, 3 * rank, win), bf16),
            *[vec((reps // 2,) + f.shape, bf16) for f in factors],
            *[vec((reps,) + f.shape, bf16) for f in factors],
            vec((seqs, head_dim), f32),
            vec((seqs, width), f32),
            vec((2, seqs, kv_local * head_dim), f32),
            vec((seqs, 3 * rank), f32),
            vec((seqs, 3 * rank), bf16),
            vec((n, seqs, 3 * rank), bf16),
            vec((rows, head_dim), f32),
            vec((rows, head_dim), f32),
            vec((rows, head_dim), f32),
            vec((rows, head_dim), f32),
            vec((seqs, width), bf16),
            vec((seqs, rank), bf16),
            vec((n, seqs, rank), bf16),
            vec((waves, slots, seqs // waves, half_w), bf16),
            vec((waves, slots, seqs // waves, half_w), bf16),
            dma,
            dma((steps,)),
            dma((steps,)),
            dma((2 * n,)),
            dma((parts,)),
            dma((parts,)),
            dma((1 + len(factors),)),
            dma((reps // 2,)),
            dma((reps,)),
            dma((reps // 2,)),
            dma((len(factors), reps // 2)),
            dma((len(factors), reps // 2)),
            dma((len(factors), reps)),
            dma((len(factors), reps)),
            dma((len(factors), reps)),
            dma((n,)),
            dma((n,)),
            dma((n,)),
            dma((n,)),
            dma((waves, slots)),
            dma((waves, slots)),
        ],
        compiler_params=pltpu.CompilerParams(
            collective_id=0, has_side_effects=True, vmem_limit_bytes=66000000
        ),
    )(
        hidden,
        norm_gain.reshape(1, -1),
        query_weight_matrix,
        key_value_weight,
        output_weight_matrix,
        down,
        *factors,
        cache_keys,
        cache_values,
        lengths,
    )


def solution(mesh):
    return jax.shard_map(
        local,
        mesh=mesh,
        in_specs=(
            P("rep", None),
            P(),
            P(None, "tp"),
            P(None, None, "tp"),
            P("tp", None),
            P(None, ("rep", "tp"), None),
            P(None, ("rep", "tp")),
            P(None, None, ("rep", "tp")),
            P(("rep", "tp"), None),
            P(None, ("rep", "tp")),
            P("rep", "tp", None, None),
            P("rep", "tp", None, None),
            P("rep"),
        ),
        out_specs=P("rep", "tp"),
        check_vma=False,
    )
```

```python
import functools
import math

import jax
import jax.numpy as jnp
from jax import lax
from jax.experimental import pallas as pl
from jax.experimental.pallas import tpu as pltpu
from jax.sharding import PartitionSpec as P

epsilon = 1e-06
rope_base = 1000000.0
adapter_scale = 0.5

f32 = jnp.float32
bf16 = jnp.bfloat16
LANES = 128
MESH_ID = pl.DeviceIdType.MESH


def nt_dot(left, right):
    return lax.dot_general(
        left, right, (((1,), (1,)), ((), ())), preferred_element_type=f32
    )


def nn_dot(left, right):
    return jnp.dot(left, right, preferred_element_type=f32)


def channels_of(n):
    return ((1, 0, n // 2), (-1, 1, n // 2), (1, 1, n // 2 - 1), (-1, 0, n // 2 - 1))


def kernel(
    dims,
    hidden,
    gain,
    wq,
    wkv,
    wo,
    dn_own,
    f_q,
    f_kv,
    f_od,
    f_ou,
    cache_k,
    cache_v,
    lengths,
    out,
    hid_b,
    norm_b,
    wq_b,
    wkv_b,
    wo_b,
    k_b,
    v_b,
    dn_b,
    a_q,
    a_kv,
    a_od,
    a_ou,
    g_q,
    g_kv,
    g_od,
    g_ou,
    angle,
    q_acc,
    kv_acc,
    inner_o,
    inner_s,
    inner_r,
    q3,
    nk3,
    nv3,
    c3,
    ctx,
    mid_s,
    mid_r,
    rs_s,
    rs_r,
    hid_sem,
    w_sem,
    kv_sem,
    wo_sem,
    k_sem,
    v_sem,
    own_sem,
    dn_ssem,
    dn_rsem,
    dn_fsem,
    a_ssem,
    a_rsem,
    g_ssem,
    g_rsem,
    g_fsem,
    in_ssem,
    in_rsem,
    mid_ssem,
    mid_rsem,
    rs_ssem,
    rs_rsem,
):
    n, reps = dims["tp"], dims["rep"]
    seqs, depth = hidden.shape
    head_dim = cache_k.shape[3]
    kv_local = cache_k.shape[1]
    heads = wq.shape[1] // head_dim
    group = heads // kv_local
    pad_heads = q3.shape[0] // seqs
    rank = dims["rank"]
    block, win = dims["block"], dims["win"]
    half_reps = reps // 2
    r = lax.axis_index("rep")
    t = lax.axis_index("tp")
    core = lax.rem(r, 2)
    partner = r + 1 - 2 * core

    own_dn = pltpu.make_async_copy(dn_own, dn_b.at[r], own_sem.at[0])
    mine_at = r // 2
    spread = (a_q, a_kv, a_od, a_ou)
    gathered = (g_q, g_kv, g_od, g_ou)
    own_f = [
        pltpu.make_async_copy(src, dst.at[mine_at], own_sem.at[1 + f])
        for f, (src, dst) in enumerate(zip((f_q, f_kv, f_od, f_ou), spread))
    ]
    own_dn.start()
    for c in own_f:
        c.start()
    hid = pltpu.make_async_copy(hidden, hid_b, hid_sem)
    hid.start()
    steps = w_sem.shape[0]
    kc = depth // steps

    def w_copies(i):
        rows = pl.ds(pl.multiple_of(i * kc, kc), kc)
        return (
            pltpu.make_async_copy(wq.at[rows, :], wq_b.at[rows, :], w_sem.at[i]),
            pltpu.make_async_copy(wkv.at[:, rows, :], wkv_b.at[:, rows, :], kv_sem.at[i]),
        )

    @pl.loop(0, steps)
    def _(i):
        for c in w_copies(i):
            c.start()

    parts = k_sem.shape[0]
    ps = seqs // parts

    def cache_copies(i):
        rows = pl.ds(i * ps, ps)
        return (
            pltpu.make_async_copy(cache_k.at[rows], k_b.at[rows], k_sem.at[i]),
            pltpu.make_async_copy(cache_v.at[rows], v_b.at[rows], v_sem.at[i]),
        )

    @pl.loop(0, parts)
    def _(i):
        for c in cache_copies(i):
            c.start()

    wide = wo.shape[1] // n
    half_w = wide // 2

    def out_cols(k, half):
        d = lax.rem(t + k + n, n)
        return pl.ds(pl.multiple_of(d * wide + half * half_w, LANES), half_w)

    def wo_copy(k, half):
        cols = out_cols(k, half)
        idx = (k % n) * 2 + half
        return pltpu.make_async_copy(wo.at[:, cols], wo_b.at[idx], wo_sem.at[idx])

    sends = []
    for k in range(n // 2, 0, -1):
        for fresh in (True, False):
            for ci, (way, half, hops) in enumerate(channels_of(n)):
                if k <= hops and (k == hops) == fresh:
                    sends.append((ci, way, half, hops, k))
    for _ci, way, half, _hops, k in sends:
        wo_copy(way * k, half).start()
    wo_copy(0, 0).start()
    wo_copy(0, 1).start()

    barrier = pltpu.get_barrier_semaphore()

    def greet(rr, tt):
        pl.semaphore_signal(barrier, inc=1, device_id=(rr, tt), device_id_type=MESH_ID)

    count = 0
    greet(partner, t)
    count += 1
    for j in range(1, n):
        greet(r, lax.rem(t + j, n))
        count += 1
    for j in range(1, half_reps):
        greet(lax.rem(r + 2 * j, reps), t)
        count += 1

    pl.semaphore_wait(barrier, count)

    def remote(src, dst, ssem, rsem, rr, tt):
        return pltpu.make_async_remote_copy(
            src_ref=src,
            dst_ref=dst,
            send_sem=ssem,
            recv_sem=rsem,
            device_id=(rr, tt),
            device_id_type=MESH_ID,
        )

    own_dn.wait()
    dn_sends = []
    for j in range(1, half_reps):
        dn_sends.append(
            remote(
                dn_b.at[r], dn_b.at[r], dn_ssem.at[j], dn_rsem.at[r],
                lax.rem(r + 2 * j, reps), t,
            )
        )
    dn_sends.append(
        remote(dn_b.at[r], dn_b.at[r], dn_fsem.at[0], dn_rsem.at[r], partner, t)
    )
    for c in dn_sends:
        c.start()
    a_sends = []

    def to_chips(f):
        buf = spread[f]
        own_f[f].wait()
        for j in range(1, half_reps):
            c = remote(
                buf.at[mine_at], buf.at[mine_at], a_ssem.at[f, j], a_rsem.at[f, mine_at],
                lax.rem(r + 2 * j, reps), t,
            )
            c.start()
            a_sends.append(c)

    to_chips(0)
    to_chips(1)
    per_plane = reps // n
    groups = per_plane // 2
    g_sends = []

    def to_planes(f):
        buf, full = spread[f], gathered[f]
        for j in range(1, half_reps):
            src = lax.rem(r + 2 * j, reps) // 2
            remote(
                buf.at[src], buf.at[src], a_ssem.at[f, j], a_rsem.at[f, src], r, t
            ).wait_recv()
        for i in range(groups):
            s = n * (2 * i + core) + t
            for j in range(1, n):
                plane = lax.rem(t + j, n)
                src = (plane * per_plane + 2 * i) // 2
                c = remote(
                    buf.at[src], full.at[s], g_ssem.at[f, i * n + j], g_rsem.at[f, s],
                    r, plane,
                )
                c.start()
                g_sends.append(c)
            src = (t * per_plane + 2 * i) // 2
            pltpu.make_async_copy(buf.at[src], full.at[s], g_rsem.at[f, s]).start()

    def across(f):
        full = gathered[f]
        for i in range(groups):
            for z in range(n):
                s = n * (2 * i + core) + z
                pltpu.make_async_copy(spread[f].at[0], full.at[s], g_rsem.at[f, s]).wait()
                c = remote(
                    full.at[s], full.at[s], g_fsem.at[f, i * n + z], g_rsem.at[f, s],
                    partner, t,
                )
                c.start()
                g_sends.append(c)

    def settled(f):
        full = gathered[f]
        for i in range(groups):
            for z in range(n):
                s = n * (2 * i + 1 - core) + z
                pltpu.make_async_copy(spread[f].at[0], full.at[s], g_rsem.at[f, s]).wait()

    half_dim = head_dim // 2
    step = lax.rem(lax.broadcasted_iota(jnp.int32, (1, head_dim), 1), half_dim)
    frequency = jnp.exp(step.astype(f32) * (-2.0 * math.log(rope_base) / head_dim))

    @pl.loop(0, seqs // 8)
    def _(i):
        for b in range(8):
            angle[pl.ds(i * 8 + b, 1), :] = lengths[i * 8 + b].astype(f32) * frequency

    hid.wait()

    @pl.loop(0, seqs // 16)
    def _(i):
        rows = pl.ds(pl.multiple_of(i * 16, 16), 16)
        x = hid_b[rows, :].astype(f32)
        square = jnp.mean(x * x, axis=-1, keepdims=True)
        norm_b[rows, :] = (
            x * lax.rsqrt(square + epsilon) * gain[...].astype(f32).reshape(1, depth)
        ).astype(bf16)

    q_acc[...] = jnp.zeros_like(q_acc)
    kv_acc[...] = jnp.zeros_like(kv_acc)

    def project(lo, hi):
        @pl.loop(lo, hi)
        def _(i):
            for c in w_copies(i):
                c.wait()
            rows = pl.ds(pl.multiple_of(i * kc, kc), kc)
            x = norm_b[:, rows]
            q_acc[...] += nn_dot(x, wq_b[rows, :])
            for j in range(2):
                kv_acc[j] += nn_dot(x, wkv_b[j, rows, :])

    project(0, steps // 4)
    dn_fwd = []
    for j in range(half_reps - 1, 0, -1):
        src = lax.rem(r + 2 * j, reps)
        remote(dn_b.at[src], dn_b.at[src], dn_fsem.at[j], dn_rsem.at[src], partner, t).wait_recv()
        c = remote(dn_b.at[src], dn_b.at[src], dn_fsem.at[j], dn_rsem.at[src], partner, t)
        c.start()
        dn_fwd.append(c)
    to_planes(0)
    to_planes(1)
    project(steps // 4, steps // 2)

    for j in range(half_reps):
        src = lax.rem(partner + 2 * j, reps)
        remote(dn_b.at[src], dn_b.at[src], dn_fsem.at[j], dn_rsem.at[src], partner, t).wait_recv()

    part = jnp.zeros((seqs, 3 * rank), f32)
    for j in range(reps):
        start = (j * n + t) * block
        cols = pl.ds(pl.multiple_of(start // win * win, LANES), win)
        part = part + nt_dot(norm_b[:, cols], dn_b[j])
    inner_s[...] = part.astype(bf16)
    inner_o[...] = part
    in_sends = []
    for j in range(1, n):
        c = remote(
            inner_s, inner_r.at[j], in_ssem.at[j], in_rsem.at[j], r, lax.rem(t + j, n)
        )
        c.start()
        in_sends.append(c)

    across(0)
    across(1)
    to_chips(2)
    to_chips(3)
    project(steps // 2, 3 * steps // 4)
    to_planes(2)
    to_planes(3)
    project(3 * steps // 4, steps)
    settled(0)
    settled(1)

    total = inner_o[...]
    for c in in_sends:
        c.wait_recv()
    for j in range(1, n):
        total = total + inner_r[j].astype(f32)
    inner = total.astype(bf16).astype(f32)
    inner_q = inner[:, :rank].astype(bf16)
    inner_k = inner[:, rank : 2 * rank].astype(bf16)
    inner_v = inner[:, 2 * rank :].astype(bf16)

    def rows_of(j):
        w = g_kv.shape[2]
        return g_kv[:, j].astype(f32).reshape(reps * w, rank).astype(bf16)

    q_up = jnp.concatenate([g_q[s] for s in range(reps)], axis=1)
    q = q_acc[...] + adapter_scale * nn_dot(inner_q, q_up)
    nk = kv_acc[0] + adapter_scale * nt_dot(inner_k, rows_of(0))
    nv = kv_acc[1] + adapter_scale * nt_dot(inner_v, rows_of(1))

    across(2)
    across(3)

    cosv = jnp.cos(angle[...])
    sinv = jnp.sin(angle[...])
    lane = lax.broadcasted_iota(jnp.int32, (seqs, head_dim), 1)
    sinv = jnp.where(lane < half_dim, -sinv, sinv)

    def turn(x):
        return x * cosv + pltpu.roll(x, head_dim // 2, 1) * sinv

    for h in range(pad_heads):
        rows = pl.ds(h, seqs, stride=pad_heads)
        if h < heads:
            q3[rows, :] = turn(q[:, h * head_dim : (h + 1) * head_dim])
        else:
            q3[rows, :] = jnp.zeros((seqs, head_dim), f32)
    for j in range(kv_local):
        key = turn(nk[:, j * head_dim : (j + 1) * head_dim]).astype(bf16).astype(f32)
        val = nv[:, j * head_dim : (j + 1) * head_dim].astype(bf16).astype(f32)
        for g in range(pad_heads):
            if min(g // group, kv_local - 1) == j:
                rows = pl.ds(g, seqs, stride=pad_heads)
                nk3[rows, :] = key
                nv3[rows, :] = val

    cache = cache_k.shape[2]
    span = kv_local * cache
    score_scale = 1.0 / math.sqrt(head_dim)
    bs = min(16, ps)
    per = ps // bs

    def attend(i):
        @pl.when(lax.rem(i, per) == 0)
        def _():
            for c in cache_copies(i // per):
                c.wait()

        base = pl.multiple_of(i * (bs * pad_heads), bs * pad_heads)
        rows = pl.ds(base, bs * pad_heads)
        qq = q3[rows, :]
        hi = qq.astype(bf16).astype(f32)
        rest = qq - hi
        mid = rest.astype(bf16).astype(f32)
        low = rest - mid
        own = jnp.sum(qq * nk3[rows, :], axis=-1, keepdims=True) * score_scale
        row_id = lax.broadcasted_iota(jnp.int32, (pad_heads, span), 0)
        col_id = lax.broadcasted_iota(jnp.int32, (pad_heads, span), 1)
        mine = jnp.minimum(row_id // group, kv_local - 1) == col_id // cache
        pos = lax.rem(col_id, cache)
        scored = []
        for b in range(bs):
            sl = slice(b * pad_heads, (b + 1) * pad_heads)
            stack = jnp.concatenate([hi[sl], mid[sl], low[sl]], axis=0).astype(bf16)
            keys = k_b[i * bs + b].reshape(span, head_dim)
            dots = nt_dot(stack, keys)
            sc = (
                dots[:pad_heads]
                + dots[pad_heads : 2 * pad_heads]
                + dots[2 * pad_heads :]
            ) * score_scale
            live = jnp.logical_and(mine, pos < lengths[i * bs + b])
            scored.append(jnp.where(live, sc, -1e30))
        sc = jnp.concatenate(scored, axis=0)
        top = jnp.maximum(jnp.max(sc, axis=-1, keepdims=True), own)
        w = jnp.exp(sc - top)
        ow = jnp.exp(own - top)
        scale = 1.0 / (jnp.sum(w, axis=-1, keepdims=True) + ow)
        probs = w * scale
        own_part = (ow * scale).astype(bf16).astype(f32) * nv3[rows, :]
        for b in range(bs):
            sl = slice(b * pad_heads, (b + 1) * pad_heads)
            vals = v_b[i * bs + b].reshape(span, head_dim)
            here = pl.ds(base + b * pad_heads, pad_heads)
            c3[here, :] = nn_dot(probs[sl].astype(bf16), vals) + own_part[sl]

    waves = rs_s.shape[0]
    ws = seqs // waves

    def attend_wave(wave):
        pl.loop(wave * ws // bs, (wave + 1) * ws // bs)(attend)
        for h in range(heads):
            ctx[wave * ws : (wave + 1) * ws, h * head_dim : (h + 1) * head_dim] = c3[
                pl.ds(wave * ws * pad_heads + h, ws, stride=pad_heads), :
            ].astype(bf16)

    tile = min(512, half_w)
    offsets = []
    at = 0
    for _way, _half, hops in channels_of(n):
        offsets.append(at)
        at += hops
    rs_sends = []

    def hop(wave, place, way):
        return remote(
            rs_s.at[wave, place], rs_r.at[wave, place], rs_ssem.at[wave, place],
            rs_rsem.at[wave, place], r, lax.rem(t + way + n, n),
        )

    def pass_on(wave, ci, way, half, hops, k):
        idx = ((way * k) % n) * 2 + half
        place = offsets[ci] + k - 1
        if wave == 0:
            wo_copy(way * k, half).wait()
        if k < hops:
            hop(wave, place + 1, way).wait_recv()

        @pl.loop(0, half_w // tile)
        def _(i):
            cols = pl.ds(pl.multiple_of(i * tile, tile), tile)
            value = nn_dot(ctx[wave * ws : (wave + 1) * ws, :], wo_b[idx, :, cols])
            if k < hops:
                value = value + rs_r[wave, place + 1, :, cols].astype(f32)
            rs_s[wave, place, :, cols] = value.astype(bf16)

        c = hop(wave, place, way)
        c.start()
        rs_sends.append((c, k))

    early = [x for x in sends if x[3] == x[4] == n // 2]
    lone = [x for x in sends if x[3] == x[4] != n // 2]
    joined = [x for x in sends if x[3] != x[4]]
    attend_wave(0)
    for x in early + lone:
        pass_on(0, *x)
    for wave in range(1, waves):
        attend_wave(wave)
        for x in early:
            pass_on(wave, *x)
        for x in joined:
            pass_on(wave - 1, *x)
        for x in lone:
            pass_on(wave, *x)

    settled(2)
    settled(3)
    down_t = jnp.concatenate([g_od[s] for s in range(reps)], axis=1)
    total_mid = nt_dot(ctx[...], down_t)
    mid_s[...] = total_mid.astype(bf16)
    mid_sends = []
    for j in range(1, n):
        c = remote(mid_s, mid_r.at[j], mid_ssem.at[j], mid_rsem.at[j], r, lax.rem(t + j, n))
        c.start()
        mid_sends.append(c)
    for x in joined:
        pass_on(waves - 1, *x)

    for c in mid_sends:
        c.wait_recv()
    for j in range(1, n):
        total_mid = total_mid + mid_r[j].astype(f32)
    middle = total_mid.astype(bf16)
    up_full = jnp.concatenate([g_ou[s] for s in range(reps)], axis=1)
    final = []
    for half in range(2):
        wo_copy(0, half).wait()
        final.append(
            nn_dot(ctx[...], wo_b[half])
            + adapter_scale * nn_dot(middle, up_full[:, half * half_w : (half + 1) * half_w])
        )
    for c, k in rs_sends:
        if k == 1:
            c.wait_recv()
    for half in range(2):
        value = final[half]
        for ci, (_way, h2, hops) in enumerate(channels_of(n)):
            if h2 == half and hops > 0:
                value = value + rs_r[:, offsets[ci]].reshape(seqs, half_w).astype(f32)
        out[:, half * half_w : (half + 1) * half_w] = value.astype(bf16)

    for c in dn_sends + dn_fwd + a_sends + g_sends + in_sends + mid_sends:
        c.wait_send()
    for c, _k in rs_sends:
        c.wait_send()


def local(
    hidden,
    norm_gain,
    query_weight_matrix,
    key_value_weight,
    output_weight_matrix,
    input_down_factors,
    query_up_factor,
    key_value_up_factors,
    output_down_factor,
    output_up_factor,
    cache_keys,
    cache_values,
    lengths,
):
    reps, n = lax.axis_size("rep"), lax.axis_size("tp")
    r, t = lax.axis_index("rep"), lax.axis_index("tp")
    seqs, depth = hidden.shape
    _, kv_local, cache, head_dim = cache_keys.shape
    width = query_weight_matrix.shape[1]
    heads = width // head_dim
    rank = input_down_factors.shape[2]
    block = input_down_factors.shape[1]
    win = max(block, LANES)

    down = jnp.swapaxes(input_down_factors, 1, 2).reshape(3 * rank, block)
    if win != block:
        spot = lax.rem((r * n + t) * block, win)
        down = lax.dynamic_update_slice(
            jnp.zeros((3 * rank, win), down.dtype), down, (0, spot)
        )
    f_q = query_up_factor
    f_kv = jnp.swapaxes(key_value_up_factors, 1, 2)
    f_od = output_down_factor.T
    f_ou = output_up_factor
    factors = (f_q, f_kv, f_od, f_ou)
    dims = dict(
        tp=n, rep=reps, rank=rank, block=block, win=win,
    )
    pad_heads = -(-heads // 8) * 8
    wide = depth // n
    half_w = wide // 2
    rows = seqs * pad_heads
    slots = sum(hops for _, _, hops in channels_of(n))
    steps, parts, waves = 16, 4, 2
    dma = pltpu.SemaphoreType.DMA
    hbm = pl.BlockSpec(memory_space=pl.ANY)
    vmem = pl.BlockSpec(memory_space=pltpu.VMEM)
    smem = pl.BlockSpec(memory_space=pltpu.SMEM)
    vec = pltpu.VMEM
    return pl.pallas_call(
        functools.partial(kernel, dims),
        name="decode_block",
        out_shape=jax.ShapeDtypeStruct((seqs, wide), bf16),
        in_specs=[hbm, vmem] + [hbm] * 10 + [smem],
        out_specs=vmem,
        scratch_shapes=[
            vec((seqs, depth), bf16),
            vec((seqs, depth), bf16),
            vec((depth, width), bf16),
            vec((2, depth, kv_local * head_dim), bf16),
            vec((2 * n, width, half_w), bf16),
            vec((seqs, kv_local, cache, head_dim), bf16),
            vec((seqs, kv_local, cache, head_dim), bf16),
            vec((reps, 3 * rank, win), bf16),
            *[vec((reps // 2,) + f.shape, bf16) for f in factors],
            *[vec((reps,) + f.shape, bf16) for f in factors],
            vec((seqs, head_dim), f32),
            vec((seqs, width), f32),
            vec((2, seqs, kv_local * head_dim), f32),
            vec((seqs, 3 * rank), f32),
            vec((seqs, 3 * rank), bf16),
            vec((n, seqs, 3 * rank), bf16),
            vec((rows, head_dim), f32),
            vec((rows, head_dim), f32),
            vec((rows, head_dim), f32),
            vec((rows, head_dim), f32),
            vec((seqs, width), bf16),
            vec((seqs, rank), bf16),
            vec((n, seqs, rank), bf16),
            vec((waves, slots, seqs // waves, half_w), bf16),
            vec((waves, slots, seqs // waves, half_w), bf16),
            dma,
            dma((steps,)),
            dma((steps,)),
            dma((2 * n,)),
            dma((parts,)),
            dma((parts,)),
            dma((1 + len(factors),)),
            dma((reps // 2,)),
            dma((reps,)),
            dma((reps // 2,)),
            dma((len(factors), reps // 2)),
            dma((len(factors), reps // 2)),
            dma((len(factors), reps)),
            dma((len(factors), reps)),
            dma((len(factors), reps)),
            dma((n,)),
            dma((n,)),
            dma((n,)),
            dma((n,)),
            dma((waves, slots)),
            dma((waves, slots)),
        ],
        compiler_params=pltpu.CompilerParams(
            collective_id=0, has_side_effects=True, vmem_limit_bytes=66000000
        ),
    )(
        hidden,
        norm_gain,
        query_weight_matrix,
        key_value_weight,
        output_weight_matrix,
        down,
        *factors,
        cache_keys,
        cache_values,
        lengths,
    )


def solution(mesh):
    return jax.shard_map(
        local,
        mesh=mesh,
        in_specs=(
            P("rep", None),
            P(),
            P(None, "tp"),
            P(None, None, "tp"),
            P("tp", None),
            P(None, ("rep", "tp"), None),
            P(None, ("rep", "tp")),
            P(None, None, ("rep", "tp")),
            P(("rep", "tp"), None),
            P(None, ("rep", "tp")),
            P("rep", "tp", None, None),
            P("rep", "tp", None, None),
            P("rep"),
        ),
        out_specs=P("rep", "tp"),
        check_vma=False,
    )
```
